256 devices in a mesh: seq: 64 (over x, z, core), head: 4 (over y).
Axes of the slice: x: 4, y: 4, z: 8, core: 2. Of those that a mesh axis runs over, the one named last changes fastest.
Arguments:
- x_in: bfloat16 [65536, 4096], P('seq', 'head'), may hold values from -6 to 6
- z_gate: bfloat16 [65536, 4096], P('seq', 'head'), may hold values from -6 to 6
- b_in: bfloat16 [65536, 128], P('seq', 'head'), may hold values from -2 to 2
- c_in: bfloat16 [65536, 128], P('seq', 'head'), may hold values from -2 to 2
- dt_raw: float32 [65536, 64], P('seq', 'head'), may hold values from -4 to 4
- decay_rate: float32 [64], P('head'), may hold values from 7.6293945e-06 to 0.05, as said below
- skip_gain: float32 [64], P('head'), may hold values from 0.5 to 1.5
- norm_gain: float32 [4096], P('head'), may hold values from 0.1 to 1.9
- w_out: bfloat16 [4096, 2560], P('head'), may hold values from -0.09375 to 0.09375
- doc_lengths: int32 [32], replicated, may hold values from 1 to 16384, 65536 in all
Outputs:
- mixed: bfloat16 [65536, 2560], P(('seq', 'head'))
The draws below stay inside these ranges and needn't reach their ends.
Inputs may be any that keep to these rules, and one draw needn't show every extreme that they name: `decay_rate`: every head's rate lies in the range. `doc_lengths`: they sum to 65536; the longest is exactly 16384.
All inputs are finite; a program needn't handle non-finite values.
Results may differ from the reference program's by a relative error of at most 0.018.
Values may be sent and summed in bfloat16 or wider, within the bound.
A program may use at most 128 MiB of HBM per device.

```python
import math
import jax
import jax.numpy as jnp
import numpy as np
from jax import lax

D = 2560
HEADS = 64
HEAD_DIM = 64
STATE = 128
SPAN = 256
DOCS = 32
TOKENS = 65536
DOC_MOST = 16384
N_HEAD = 4


def draw_decay_rate(key, part):
    uniform_draw = jax.random.uniform(jax.random.fold_in(key, 11), (HEADS,), jnp.float32)
    lowest = 0.5 / TOKENS
    highest = 0.05
    return jnp.exp(jnp.log(lowest) + uniform_draw * (jnp.log(highest) - jnp.log(lowest))).astype(jnp.float32)


def block_levels(stream_key, shape, cuts, low, high):
    factor_of = 1.0
    for axis_at, blocks in cuts:
        draws = jax.random.uniform(jax.random.fold_in(jax.random.fold_in(stream_key, 6), axis_at), (blocks,), jnp.float32, low / len(cuts), high / len(cuts))
        factor_of = factor_of * jnp.repeat(jnp.exp(draws), shape[axis_at] // blocks).reshape((-1,) + (1,) * (len(shape) - 1 - axis_at))
    return factor_of


def split_up(number_of, total, limit, lean):
    weights = [(1 << 20) // math.isqrt(rank ** lean) + 1 for rank in range(2, number_of + 1)]
    rest, given = total - limit - (number_of - 1), [1] * (number_of - 1)
    while rest > 0:
        movable = [i for i in range(number_of - 1) if given[i] < limit]
        mass, left = sum([weights[i] for i in movable]), rest
        for i in movable:
            extra = min(limit - given[i], max(1, left * weights[i] // mass), rest)
            given[i] = given[i] + extra
            rest = rest - extra
    return np.array([limit] + given)


def uneven_parts(rng, number_of, total, most, slope):
    if number_of == 2:
        one = jax.random.randint(rng, (), max(1, total - most), min(most, total - 1) + 1)
        return jnp.stack([one, total - one])
    sizes = jnp.asarray(split_up(number_of, total, most, slope), jnp.int32)
    twos = (number_of - 1) // 2
    giver, sink = sizes[1:1 + 2 * twos:2], sizes[2:2 + 2 * twos:2]
    margin = jnp.minimum(giver - 1, most - sink)
    shifted = jax.random.randint(jax.random.fold_in(rng, 1), (twos,), 0, 1 << 20) % (margin + 1)
    sizes = sizes.at[1:1 + 2 * twos:2].set(giver - shifted).at[2:2 + 2 * twos:2].set(sink + shifted)
    return sizes[jax.random.permutation(jax.random.fold_in(rng, 2), number_of)]


def bell_draw(key, extent, spread, limit, shards=(), kind=jnp.bfloat16):
    entries = jax.random.normal(key, extent, jnp.float32) * spread
    if len(shards) > 0:
        entries = block_levels(key, extent, shards, -0.22, 0.18) * entries
    return jnp.clip(entries, min=-limit, max=limit).astype(kind)


def setup_inputs(seed: int = 0) -> dict:
    splits = jax.random.split(jax.random.key(seed), 11)
    return {
        "x_in": bell_draw(splits[0], (TOKENS, HEADS * HEAD_DIM), 1.0, 6.0, ((0, 64), (1, 4))),
        "z_gate": bell_draw(splits[1], (TOKENS, HEADS * HEAD_DIM), 1.0, 6.0, ((0, 64), (1, 4))),
        "b_in": bell_draw(splits[2], (TOKENS, STATE), 0.3, 2.0, ((0, 64), (1, 4))),
        "c_in": bell_draw(splits[3], (TOKENS, STATE), 0.3, 2.0, ((0, 64), (1, 4))),
        "dt_raw": bell_draw(splits[4], (TOKENS, HEADS), 1.0, 4.0, ((0, 64), (1, 4)), jnp.float32),
        "decay_rate": draw_decay_rate(jax.random.fold_in(splits[10], 71), 0),
        "skip_gain": jnp.clip(0.5 + 1.0 * jax.random.uniform(splits[6], (HEADS,), jnp.float32) ** block_levels(splits[6], (HEADS,), ((0, 4),), -0.2, 0.2), 0.5, 1.5),
        "norm_gain": jnp.clip(1.0 + 0.18 * jax.random.normal(splits[7], (HEADS * HEAD_DIM,), jnp.float32), 0.1, 1.9),
        "w_out": bell_draw(splits[8], (HEADS * HEAD_DIM, D), (HEADS * HEAD_DIM) ** -0.5, 0.09375, ((0, 4),)),
        "doc_lengths": uneven_parts(splits[9], DOCS, TOKENS, DOC_MOST, 2).astype(jnp.int32),
    }


norm_eps = 1e-05

def reference(x_in, z_gate, b_in, c_in, dt_raw, decay_rate, skip_gain, norm_gain, w_out, doc_lengths):
    inner_width = HEADS * HEAD_DIM
    block_width = inner_width // N_HEAD
    positions = jnp.arange(TOKENS, dtype=jnp.int32)
    doc_ends = jnp.cumsum(doc_lengths).astype(jnp.int32)
    doc_starts = (doc_ends - doc_lengths).astype(jnp.int32)
    doc_ids = lax.optimization_barrier(jnp.sum((positions[:, None] >= doc_ends[None, :]).astype(jnp.int32), axis=1)).astype(jnp.int32)
    start_flags = jnp.any(positions[:, None] == doc_starts[None, :], axis=1).astype(jnp.int32)
    step_size = jax.nn.softplus(dt_raw)
    log_decay = -step_size * decay_rate[None, :]
    spans = TOKENS // SPAN
    inputs = x_in.reshape(spans, SPAN, HEADS, HEAD_DIM)
    gates = z_gate.reshape(spans, SPAN, inner_width)
    b_blocks = b_in.reshape(spans, SPAN, STATE)
    c_blocks = c_in.reshape(spans, SPAN, STATE)
    step_blocks = step_size.reshape(spans, SPAN, HEADS)
    decay_blocks = log_decay.reshape(spans, SPAN, HEADS)
    id_blocks = doc_ids.reshape(spans, SPAN)
    flag_blocks = start_flags.reshape(spans, SPAN)
    w_blocks = w_out.astype(jnp.float32).reshape(N_HEAD, block_width, D)
    local_pos = jnp.arange(SPAN, dtype=jnp.int32)
    causal_mask = local_pos[:, None] >= local_pos[None, :]

    def span_step(carried, pieces):
        xc, zc, bc, cc, steps_here, decay_here, ids_here, flags_here = pieces
        cumulative = jnp.cumsum(decay_here, axis=0)
        scores = jnp.dot(cc, bc.T, preferred_element_type=jnp.float32)
        same_doc = causal_mask & (ids_here[:, None] == ids_here[None, :])
        cum_heads = cumulative.T
        differ = cum_heads[:, :, None] - cum_heads[:, None, :]
        decay_table = jnp.exp(jnp.where(same_doc[None], differ, -jnp.inf))
        weights = (scores[None] * decay_table * steps_here.T[:, None, :]).astype(jnp.bfloat16)
        y_local = jnp.einsum('hij,jhp->ihp', weights.astype(jnp.float32), xc.astype(jnp.float32))
        unreset = (jnp.cumsum(flags_here) == 0).astype(jnp.float32)
        from_start = jnp.exp(cumulative) * unreset[:, None]
        y_inter = jnp.einsum('in,hpn->ihp', cc.astype(jnp.float32), carried, precision=lax.Precision.HIGHEST) * from_start[:, :, None]
        y_total = y_local + y_inter + skip_gain[None, :, None] * xc.astype(jnp.float32)
        to_end = jnp.exp(cumulative[-1][None, :] - cumulative) * (ids_here == ids_here[-1])[:, None].astype(jnp.float32)
        scaled = (xc.astype(jnp.float32) * (to_end * steps_here)[:, :, None]).astype(jnp.bfloat16)
        block_state = jnp.einsum('jhp,jn->hpn', scaled.astype(jnp.float32), bc.astype(jnp.float32))
        new_state = from_start[-1][:, None, None] * carried + block_state
        gated = y_total.reshape(SPAN, inner_width) * jax.nn.silu(zc.astype(jnp.float32))
        inverse_rms = lax.rsqrt(lax.optimization_barrier(jnp.mean(gated * gated, axis=1)) + norm_eps)
        normed = (gated * norm_gain[None, :]).astype(jnp.bfloat16)
        partials = jnp.einsum('qkc,kcd->kqd', normed.astype(jnp.float32).reshape(SPAN, N_HEAD, block_width), w_blocks)
        summed = lax.optimization_barrier(jnp.sum(partials.astype(jnp.bfloat16).astype(jnp.float32), axis=0))
        return (new_state, (summed * inverse_rms[:, None]).astype(jnp.bfloat16))
    initial = jnp.zeros((HEADS, HEAD_DIM, STATE), jnp.float32)
    _, out_rows = lax.scan(span_step, initial, (inputs, gates, b_blocks, c_blocks, step_blocks, decay_blocks, id_blocks, flag_blocks))
    return out_rows.reshape(TOKENS, D)
```

```python
import functools

import jax
import jax.numpy as jnp
from jax import lax
from jax.experimental import pallas as pl
from jax.experimental.pallas import tpu as pltpu
from jax.sharding import PartitionSpec as P

SPAN = 256
NORM_EPS = 1e-05
MESH = pl.DeviceIdType.MESH
F32 = jnp.float32
BF16 = jnp.bfloat16


def pieces(v, terms):
    out = []
    for _ in range(terms):
        part = v.astype(BF16)
        out.append(part)
        v = v - part.astype(F32)
    return out


def expand(v, spread, terms=2):
    total = None
    for part in pieces(v, terms):
        term = jnp.dot(part, spread, preferred_element_type=F32)
        total = term if total is None else total + term
    return total


def iota(shape, dim):
    return lax.broadcasted_iota(jnp.int32, shape, dim)


def layer_kernel(
    sizes,
    bc_ref, dt_ref, rate_ref, skip_ref, gain_ref, docs_ref, x_hbm, z_hbm, w_hbm,
    out_ref,
    x_ref, z_ref, w_ref, bt_ref, ct_ref, xf_ref, e_ref, rows_ref, before_ref, ur_ref, as_ref,
    state_ref, decay_ref, got_state, got_decay, line_ref, got_line, back_ref, inc_ref, norm_ref,
    sq_ref, got_sq, send_r, got_r, send_l, got_l,
    in_sem, bc_send, bc_recv, st_send, st_recv, dc_send, dc_recv, ln_send, ln_recv, bk_send, bk_recv,
    sq_send, sq_recv, r_send, r_recv, l_send, l_recv,
):
    n_head, n_seq, line = sizes
    rows, width = x_ref.shape
    heads = dt_ref.shape[1]
    head_size = width // heads
    state_size = bt_ref.shape[0]
    piece = bc_ref.shape[0] // 2
    spans = rows // SPAN
    me, seq = lax.axis_index("head"), lax.axis_index("seq")
    at_line, place = seq // line, seq % line
    first = seq - place
    half = width // 2
    part = state_size * 2 // line

    def load(i, src, dst):
        return pltpu.make_async_copy(src, dst, in_sem.at[i])

    loads = [load(0, x_hbm, x_ref), load(1, z_hbm, z_ref), load(2, w_hbm, w_ref)]
    for one in loads:
        one.start()

    barrier = pltpu.get_barrier_semaphore()
    for k in range(1, n_head):
        pl.semaphore_signal(barrier, inc=1, device_id={"head": (me + k) % n_head}, device_id_type=MESH)

    @pl.loop(1, line)
    def _(k):
        pl.semaphore_signal(
            barrier, inc=1, device_id={"seq": first + (place + k) % line}, device_id_type=MESH
        )

    for step in (line, n_seq - line):
        pl.semaphore_signal(barrier, inc=1, device_id={"seq": (seq + step) % n_seq}, device_id_type=MESH)
    pl.semaphore_wait(barrier, n_head - 1 + line - 1 + 2)

    def bc_copy(k, what, owner):
        dst = (bt_ref, ct_ref)[what].at[pl.ds(pl.multiple_of(owner * piece, piece), piece), :]
        return pltpu.make_async_remote_copy(
            src_ref=bc_ref.at[pl.ds(what * piece, piece), :],
            dst_ref=dst,
            send_sem=bc_send.at[what, k],
            recv_sem=bc_recv.at[what, owner],
            device_id={"head": (me + k) % n_head},
            device_id_type=MESH,
        )

    for what in range(2):
        for k in range(1, n_head):
            bc_copy(k, what, me).start()
        mine = pl.ds(pl.multiple_of(me * piece, piece), piece)
        (bt_ref, ct_ref)[what][mine, :] = bc_ref[what * piece : (what + 1) * piece, :]

    n_docs = docs_ref.shape[1]
    lengths = jnp.broadcast_to(docs_ref[...].astype(F32), (n_docs, n_docs))
    up, across = iota((n_docs, n_docs), 0), iota((n_docs, n_docs), 1)
    ends_col = jnp.sum(jnp.where(across <= up, lengths, 0.0), axis=1, keepdims=True)
    lengths_col = jnp.sum(jnp.where(across == up, lengths, 0.0), axis=1, keepdims=True)
    ends_row = jnp.sum(
        jnp.where(up <= across, jnp.broadcast_to(lengths_col, (n_docs, n_docs)), 0.0), axis=0, keepdims=True
    )

    def id_of(position):
        return jnp.sum(jnp.where(position >= ends_row, 1.0, 0.0), axis=1, keepdims=True)

    def ids_of(s):
        start = seq * rows + s * SPAN
        col = id_of((start + iota((SPAN, 1), 0)).astype(F32))
        row = jnp.sum(
            jnp.where((start + iota((1, SPAN), 1)).astype(F32) >= ends_col, 1.0, 0.0), axis=0, keepdims=True
        )
        ahead = start - 1 + iota((1, 1), 0)
        previous = id_of(ahead.astype(F32)) - jnp.where(ahead < 0, 1.0, 0.0)
        last = id_of((start + SPAN - 1 + iota((1, 1), 0)).astype(F32))
        return col, row, previous, last

    spread = (iota((heads, width), 1) // head_size == iota((heads, width), 0)).astype(BF16)
    below = (iota((SPAN, SPAN), 0) >= iota((SPAN, SPAN), 1)).astype(BF16)

    loads[0].wait()

    def scale_span(s, device_decay):
        at = pl.ds(pl.multiple_of(s * SPAN, SPAN), SPAN)
        raw = dt_ref[at, :]
        step = jnp.maximum(raw, 0.0) + jnp.log(1.0 + jnp.exp(-jnp.abs(raw)))
        cum = None
        for term in pieces(-step * rate_ref[...], 3):
            sums = jnp.dot(below, term, preferred_element_type=F32)
            cum = sums if cum is None else cum + sums
        middle = 0.5 * cum[SPAN - 1 : SPAN, :]
        e_ref[at, :] = jnp.exp(cum - middle)
        forward = step * jnp.exp(middle - cum)
        xf_ref[at, :] = (x_ref[at, :].astype(F32) * expand(forward, spread)).astype(BF16)
        _, _, previous, last = ids_of(s)
        to_middle = jnp.exp(middle)
        total = jnp.exp(2.0 * middle) * jnp.where(last == previous, 1.0, 0.0)
        both = jnp.concatenate(
            [jnp.broadcast_to(to_middle, (8, heads)), jnp.broadcast_to(total, (8, heads))], axis=0
        )
        rows_ref[pl.ds(pl.multiple_of(s * 16, 16), 16), :] = expand(both, spread, 3)
        return device_decay * total

    device_decay = lax.fori_loop(0, spans, scale_span, jnp.ones((1, heads), F32))
    decay_ref[...] = jnp.zeros_like(decay_ref)
    decay_ref[:, :heads] = jnp.broadcast_to(device_decay, (8, heads))

    def line_peer(k):
        return {"seq": first + (place + k) % line}

    def from_peer(k):
        return (place + line - k) % line

    def decay_copy(k, owner):
        return pltpu.make_async_remote_copy(
            src_ref=decay_ref,
            dst_ref=got_decay.at[owner],
            send_sem=dc_send.at[k],
            recv_sem=dc_recv.at[owner],
            device_id=line_peer(k),
            device_id_type=MESH,
        )

    @pl.loop(1, line)
    def _(k):
        decay_copy(k, place).start()

    got_decay[place] = decay_ref[...]

    for k in range(1, n_head):
        bc_copy(k, 0, (me + n_head - k) % n_head).wait_recv()

    def state_span(s, running):
        at = pl.ds(pl.multiple_of(s * SPAN, SPAN), SPAN)
        before_ref[s] = running
        _, row, _, last = ids_of(s)
        kept = jnp.where(row == last, bt_ref[:, at].astype(F32), 0.0).astype(BF16)
        sums = jnp.dot(kept, xf_ref[at, :], preferred_element_type=F32)
        base = pl.multiple_of(s * 16, 16)
        return rows_ref[pl.ds(base + 8, 1), :] * running + sums * rows_ref[pl.ds(base, 1), :]

    final = lax.fori_loop(0, spans, state_span, jnp.zeros((state_size, width), F32))
    state_ref[...] = final.astype(BF16)

    def own_part(t):
        return (
            pl.ds(pl.multiple_of((t // 2) * part, part), part),
            pl.ds(pl.multiple_of((t % 2) * half, half), half),
        )

    def state_copy(k, owner):
        to = (place + k) % line
        return pltpu.make_async_remote_copy(
            src_ref=state_ref.at[own_part(to)],
            dst_ref=got_state.at[owner],
            send_sem=st_send.at[k],
            recv_sem=st_recv.at[owner],
            device_id=line_peer(k),
            device_id_type=MESH,
        )

    @pl.loop(1, line)
    def _(k):
        state_copy(k, place).start()

    got_state[place] = state_ref[own_part(place)]

    for k in range(1, n_head):
        bc_copy(k, 1, (me + n_head - k) % n_head).wait_recv()
    loads[1].wait()
    skip_row = expand(jnp.broadcast_to(skip_ref[...], (8, heads)), spread, 3)[:1, :]

    @pl.loop(0, spans)
    def _(s):
        at = pl.ds(pl.multiple_of(s * SPAN, SPAN), SPAN)
        col, row, previous, _ = ids_of(s)
        c_here = ct_ref[:, at].T
        scores = jnp.dot(c_here, bt_ref[:, at], preferred_element_type=F32)
        seen = (col == row) & (iota((SPAN, SPAN), 0) >= iota((SPAN, SPAN), 1))
        scores = jnp.where(seen, scores, 0.0).astype(BF16)
        local = jnp.dot(scores, xf_ref[at, :], preferred_element_type=F32)
        inter = jnp.dot(c_here, before_ref[s].astype(BF16), preferred_element_type=F32)
        base = pl.multiple_of(s * 16, 16)
        out_of_middle = expand(e_ref[at, :], spread)
        from_start = rows_ref[pl.ds(base, 1), :] * jnp.where(col == previous, 1.0, 0.0)
        gate = z_ref[at, :].astype(F32)
        gate = gate / (1.0 + jnp.exp(-gate))
        y = out_of_middle * (local + from_start * inter) + skip_row * x_ref[at, :].astype(F32)
        ur_ref[at, :] = y * gate
        as_ref[at, :] = out_of_middle * from_start * gate

    @pl.loop(1, line)
    def _(k):
        decay_copy(k, from_peer(k)).wait_recv()

    @pl.loop(1, line)
    def _(k):
        state_copy(k, from_peer(k)).wait_recv()

    lanes = iota((128, half), 1) + (place % 2) * half
    spread_here = (lanes // head_size == iota((128, half), 0)).astype(BF16)
    decays = expand(got_decay[...].reshape(line * 8, 128), spread_here, 3)
    inside, inc = [], jnp.zeros((part, half), F32)
    for d in range(line):
        inside.append(inc)
        inc = decays[8 * d : 8 * d + 1, :] * inc + got_state[d].astype(F32)
    line_ref[...] = inc
    line_copy = pltpu.make_async_remote_copy(
        src_ref=line_ref,
        dst_ref=got_line,
        send_sem=ln_send,
        recv_sem=ln_recv,
        device_id={"seq": (seq + line) % n_seq},
        device_id_type=MESH,
    )
    line_copy.start()
    line_copy.wait_recv()
    factor = jnp.where(at_line + iota((1, half), 0) > 0, 1.0, 0.0)
    earlier = got_line[...]
    for d in range(line):
        back_ref[d] = (inside[d] + factor * earlier).astype(BF16)
        factor = factor * decays[8 * d : 8 * d + 1, :]

    def back_copy(k, owner):
        return pltpu.make_async_remote_copy(
            src_ref=back_ref.at[(place + k) % line],
            dst_ref=inc_ref.at[own_part(owner)],
            send_sem=bk_send.at[k],
            recv_sem=bk_recv.at[owner],
            device_id=line_peer(k),
            device_id_type=MESH,
        )

    @pl.loop(1, line)
    def _(k):
        back_copy(k, place).start()

    inc_ref[own_part(place)] = back_ref[place]

    loads[2].wait()

    @pl.loop(1, line)
    def _(k):
        back_copy(k, from_peer(k)).wait_recv()

    def finish(block):
        at = pl.ds(pl.multiple_of(block * SPAN, SPAN), SPAN)
        before = jnp.ones((1, width), F32)
        for s in range(spans - 1):
            decay = rows_ref[16 * s + 8 : 16 * s + 9, :]
            before = jnp.where(s + iota((1, width), 0) < block, before * decay, before)
        carried = (inc_ref[...].astype(F32) * before).astype(BF16)
        inter = jnp.dot(ct_ref[:, at].T, carried, preferred_element_type=F32)
        gated = ur_ref[at, :] + as_ref[at, :] * inter
        norm_ref[at, :] = (gated * gain_ref[...]).astype(BF16)
        squares = gated * gated
        folded = squares[:, :128]
        for j in range(1, width // 128):
            folded = folded + squares[:, 128 * j : 128 * (j + 1)]
        row = jnp.sum(folded.T, axis=0, keepdims=True)
        sq_ref[block] = jnp.broadcast_to(row, (8, SPAN))

    def square_copy(k, owner):
        return pltpu.make_async_remote_copy(
            src_ref=sq_ref.at[(me + k) % n_head],
            dst_ref=got_sq.at[owner],
            send_sem=sq_send.at[k],
            recv_sem=sq_recv.at[owner],
            device_id={"head": (me + k) % n_head},
            device_id_type=MESH,
        )

    out_width = out_ref.shape[1]
    parts, cut = got_r.shape[1], got_r.shape[3]

    def product(block, column):
        return jnp.dot(
            norm_ref[pl.ds(pl.multiple_of(block * SPAN, SPAN), SPAN), :],
            w_ref[:, pl.ds(pl.multiple_of(column, cut), cut)],
            preferred_element_type=F32,
        )

    def right_copy(step, j):
        return pltpu.make_async_remote_copy(
            src_ref=send_r.at[step, j],
            dst_ref=got_r.at[step, j],
            send_sem=r_send.at[step, j],
            recv_sem=r_recv.at[step, j],
            device_id={"head": (me + 1) % n_head},
            device_id_type=MESH,
        )

    def left_copy(step, j):
        return pltpu.make_async_remote_copy(
            src_ref=send_l.at[step, j],
            dst_ref=got_l.at[step, j],
            send_sem=l_send.at[step, j],
            recv_sem=l_recv.at[step, j],
            device_id={"head": (me + n_head - 1) % n_head},
            device_id_type=MESH,
        )

    ahead, behind = (me + n_head - 1) % n_head, (me + 1) % n_head
    finish(ahead)

    @pl.loop(0, parts)
    def _(j):
        send_r[0, j] = product(ahead, j * cut).astype(BF16)
        right_copy(0, j).start()

    finish(behind)

    @pl.loop(0, parts)
    def _(j):
        send_l[0, j] = product(behind, out_width // 2 + j * cut).astype(BF16)
        left_copy(0, j).start()

    for k in range(2, n_head):
        finish((me + k) % n_head) if k < n_head - 1 else finish(me)
    for k in range(1, n_head):
        square_copy(k, me).start()

    for step in range(1, n_head - 1):
        block_r, block_l = (me + 2 * n_head - 1 - step) % n_head, (me + 1 + step) % n_head

        @pl.loop(0, parts)
        def _(j):
            own = product(block_r, j * cut)
            right_copy(step - 1, j).wait_recv()
            send_r[step, j] = (own + got_r[step - 1, j].astype(F32)).astype(BF16)
            right_copy(step, j).start()
            own = product(block_l, out_width // 2 + j * cut)
            left_copy(step - 1, j).wait_recv()
            send_l[step, j] = (own + got_l[step - 1, j].astype(F32)).astype(BF16)
            left_copy(step, j).start()

    total = sq_ref[me]
    for k in range(1, n_head):
        owner = (me + n_head - k) % n_head
        square_copy(k, owner).wait_recv()
        total = total + got_sq[owner]
    inverse_rms = lax.rsqrt(total / (width * n_head) + NORM_EPS).T[:, :1]

    @pl.loop(0, parts)
    def _(j):
        last = n_head - 2
        own = product(me, j * cut)
        right_copy(last, j).wait_recv()
        own = (own + got_r[last, j].astype(F32)) * inverse_rms
        out_ref[:, pl.ds(pl.multiple_of(j * cut, cut), cut)] = own.astype(BF16)
        column = out_width // 2 + j * cut
        own = product(me, column)
        left_copy(last, j).wait_recv()
        own = (own + got_l[last, j].astype(F32)) * inverse_rms
        out_ref[:, pl.ds(pl.multiple_of(column, cut), cut)] = own.astype(BF16)

    for k in range(1, n_head):
        for what in range(2):
            bc_copy(k, what, me).wait_send()
        square_copy(k, me).wait_send()

    @pl.loop(1, line)
    def _(k):
        decay_copy(k, place).wait_send()
        state_copy(k, place).wait_send()
        back_copy(k, place).wait_send()

    line_copy.wait_send()
    for step in range(n_head - 1):

        @pl.loop(0, parts)
        def _(j):
            right_copy(step, j).wait_send()
            left_copy(step, j).wait_send()


def on_device(sizes, x_in, z_gate, b_in, c_in, dt_raw, decay_rate, skip_gain, norm_gain, w_out, doc_lengths):
    n_head, n_seq, line = sizes
    rows, width = x_in.shape
    heads = dt_raw.shape[1]
    out_width = w_out.shape[1]
    state_size = b_in.shape[1] * n_head
    spans = rows // SPAN
    bc = jnp.concatenate([b_in, c_in], axis=1).T
    part, half = state_size * 2 // line, width // 2
    parts = 5
    cut = out_width // 2 // parts
    ring = (n_head - 1, parts, rows // n_head, cut)
    vmem, anywhere = pl.BlockSpec(memory_space=pltpu.VMEM), pl.BlockSpec(memory_space=pl.ANY)
    dma = pltpu.SemaphoreType.DMA
    return pl.pallas_call(
        functools.partial(layer_kernel, sizes),
        out_shape=jax.ShapeDtypeStruct((rows // n_head, out_width), BF16),
        in_specs=[vmem] * 6 + [anywhere] * 3,
        out_specs=vmem,
        scratch_shapes=[
            pltpu.VMEM((rows, width), BF16),
            pltpu.VMEM((rows, width), BF16),
            pltpu.VMEM(w_out.shape, BF16),
            pltpu.VMEM((state_size, rows), BF16),
            pltpu.VMEM((state_size, rows), BF16),
            pltpu.VMEM((rows, width), BF16),
            pltpu.VMEM((rows, heads), F32),
            pltpu.VMEM((spans * 16, width), F32),
            pltpu.VMEM((spans, state_size, width), F32),
            pltpu.VMEM((rows, width), F32),
            pltpu.VMEM((rows, width), F32),
            pltpu.VMEM((state_size, width), BF16),
            pltpu.VMEM((8, 128), F32),
            pltpu.VMEM((line, part, half), BF16),
            pltpu.VMEM((line, 8, 128), F32),
            pltpu.VMEM((part, half), F32),
            pltpu.VMEM((part, half), F32),
            pltpu.VMEM((line, part, half), BF16),
            pltpu.VMEM((state_size, width), BF16),
            pltpu.VMEM((rows, width), BF16),
            pltpu.VMEM((n_head, 8, SPAN), F32),
            pltpu.VMEM((n_head, 8, SPAN), F32),
            pltpu.VMEM(ring, BF16),
            pltpu.VMEM(ring, BF16),
            pltpu.VMEM(ring, BF16),
            pltpu.VMEM(ring, BF16),
            dma((3,)),
            dma((2, n_head)),
            dma((2, n_head)),
            dma((line,)),
            dma((line,)),
            dma((line,)),
            dma((line,)),
            dma,
            dma,
            dma((line,)),
            dma((line,)),
            dma((n_head,)),
            dma((n_head,)),
            dma((n_head - 1, parts)),
            dma((n_head - 1, parts)),
            dma((n_head - 1, parts)),
            dma((n_head - 1, parts)),
        ],
        compiler_params=pltpu.CompilerParams(
            collective_id=0, has_side_effects=True, vmem_limit_bytes=60 * 1024 * 1024
        ),
        name="ssd_layer",
    )(
        bc,
        dt_raw,
        decay_rate[None, :],
        skip_gain[None, :],
        norm_gain[None, :],
        doc_lengths[None, :],
        x_in,
        z_gate,
        w_out,
    )


def solution(mesh):
    sizes = (mesh.shape["head"], mesh.shape["seq"], 16)
    rows = P("seq", "head")
    return jax.shard_map(
        functools.partial(on_device, sizes),
        mesh=mesh,
        in_specs=(rows, rows, rows, rows, rows, P("head"), P("head"), P("head"), P("head", None), P()),
        out_specs=P(("seq", "head"), None),
        check_vma=False,
    )
```

```python
import functools

import jax
import jax.numpy as jnp
from jax import lax
from jax.experimental import pallas as pl
from jax.experimental.pallas import tpu as pltpu
from jax.sharding import PartitionSpec as P

SPAN = 256
NORM_EPS = 1e-05
MESH = pl.DeviceIdType.MESH
F32 = jnp.float32
BF16 = jnp.bfloat16


CYCLES = (
    (0, 1, 9, 8, 16, 24, 25, 17, 18, 10, 2, 26, 27, 3, 11, 19, 20, 28, 4, 12, 13, 21, 29, 5, 6, 14, 15, 23, 22, 30, 31, 7),
    (0, 8, 15, 7, 6, 30, 29, 28, 27, 19, 18, 26, 25, 1, 2, 3, 4, 5, 13, 14, 22, 21, 20, 12, 11, 10, 9, 17, 16, 23, 31, 24),
)
CHIPS = len(CYCLES[0])
HOPS = 14
PLAN = (0, 1, 3, 2)


def around(seq):
    packed = 0
    for chip in range(CHIPS):
        for core in range(2):
            cycle = CYCLES[core]
            at = cycle.index(chip)
            after, ahead = cycle[(at + 1) % CHIPS] * 2 + core, cycle[at - 1] * 2 + core
            value = ((at * 64 + after) * 64 + ahead) * 32 + CYCLES[1 - core].index(chip)
            packed = packed + jnp.where(seq == chip * 2 + core, value, 0)
    return packed // 131072, packed // 2048 % 64, packed // 32 % 64, packed % 32


def pieces(v, terms):
    out = []
    for _ in range(terms):
        part = v.astype(BF16)
        out.append(part)
        v = v - part.astype(F32)
    return out


def expand(v, spread, terms=2):
    total = None
    for part in pieces(v, terms):
        term = lax.dot_general(part, spread, (((0,), (0,)), ((), ())), preferred_element_type=F32)
        total = term if total is None else total + term
    return total


def iota(shape, dim):
    return lax.broadcasted_iota(jnp.int32, shape, dim)


def layer_kernel(
    sizes,
    b_ref, c_ref, dt_ref, rate_ref, skip_ref, gain_ref, docs_ref, x_hbm, z_hbm, w_hbm,
    out_ref,
    x_ref, z_ref, wf_ref, bt_ref, ct_ref, xf_ref, e_ref, rows_ref, before_ref, ur_ref, as_ref,
    state_ref, decay_ref, got_state, got_decay, line_ref, got_line, back_ref, inc_ref, norm_ref,
    sq_ref, got_sq, lhs_ref, relay_ref, acc_ref,
    in_sem, bc_send, bc_recv, st_send, st_recv, dc_send, dc_recv, ln_send, ln_recv, bk_send, bk_recv,
    sq_send, sq_recv, y_send, y_recv, r_send, r_recv, l_send, l_recv, d_send, d_recv,
    a_send, a_recv, f_send, f_recv,
):
    n_head, n_seq, line = sizes
    rows, width = x_ref.shape
    heads = dt_ref.shape[0]
    head_size = width // heads
    state_size = bt_ref.shape[0]
    piece = b_ref.shape[0]
    spans = rows // SPAN
    me, seq = lax.axis_index("head"), lax.axis_index("seq")
    at_line, place = seq // line, seq % line
    first = seq - place
    half = width // 2
    part = state_size * 2 // line

    def load(i, src, dst):
        return pltpu.make_async_copy(src, dst, in_sem.at[i])

    loads = [load(0, x_hbm, x_ref), load(1, z_hbm, z_ref), load(2, w_hbm, wf_ref.at[me])]
    for one in loads:
        one.start()

    barrier = pltpu.get_barrier_semaphore()
    for k in range(1, n_head):
        pl.semaphore_signal(barrier, inc=1, device_id={"head": (me + k) % n_head}, device_id_type=MESH)

    @pl.loop(1, line)
    def _(k):
        pl.semaphore_signal(
            barrier, inc=1, device_id={"seq": first + (place + k) % line}, device_id_type=MESH
        )

    for step in (line, n_seq - line):
        pl.semaphore_signal(barrier, inc=1, device_id={"seq": (seq + step) % n_seq}, device_id_type=MESH)
    pl.semaphore_wait(barrier, n_head - 1 + line - 1 + 2)

    def bc_copy(k, what, owner):
        dst = (bt_ref, ct_ref)[what].at[pl.ds(pl.multiple_of(owner * piece, piece), piece), :]
        return pltpu.make_async_remote_copy(
            src_ref=(b_ref, c_ref)[what],
            dst_ref=dst,
            send_sem=bc_send.at[what, k],
            recv_sem=bc_recv.at[what, owner],
            device_id={"head": (me + k) % n_head},
            device_id_type=MESH,
        )

    core = seq % 2
    partner = seq + 1 - 2 * core
    spot, after, ahead_of, other_spot = around(seq // 2 * 2 + core)
    out_width = wf_ref.shape[2]
    slice_rows, side = wf_ref.shape[1] // CHIPS, out_width // 2

    def shard(n):
        return (me + (1, n_head - 1, 2)[n]) % n_head

    def chunk(owner, position, column):
        at = pl.multiple_of((position + CHIPS) % CHIPS * slice_rows, slice_rows)
        return wf_ref.at[owner, pl.ds(at, slice_rows), pl.ds(pl.multiple_of(column * side, 128), side)]

    def y_place(slot):
        return spot if slot == 0 else spot + HOPS + slot

    def y_copy(slot, k, owner):
        where = chunk(owner, y_place(slot), core)
        return pltpu.make_async_remote_copy(
            src_ref=where,
            dst_ref=where,
            send_sem=y_send.at[slot, k],
            recv_sem=y_recv.at[slot, owner],
            device_id={"head": (me + k) % n_head},
            device_id_type=MESH,
        )

    def right_copy(step, n, position):
        where = chunk(shard(n), position, core)
        return pltpu.make_async_remote_copy(
            src_ref=where,
            dst_ref=where,
            send_sem=r_send.at[step, n],
            recv_sem=r_recv.at[step, n],
            device_id={"seq": after},
            device_id_type=MESH,
        )

    def left_copy(step, n, position):
        where = chunk(shard(n), position, core)
        return pltpu.make_async_remote_copy(
            src_ref=where,
            dst_ref=where,
            send_sem=l_send.at[step, n],
            recv_sem=l_recv.at[step, n],
            device_id={"seq": ahead_of},
            device_id_type=MESH,
        )

    def partner_copy(e, n, position, column):
        where = chunk(shard(n), position, column)
        return pltpu.make_async_remote_copy(
            src_ref=where,
            dst_ref=where,
            send_sem=d_send.at[e, n],
            recv_sem=d_recv.at[e, n],
            device_id={"seq": partner},
            device_id_type=MESH,
        )

    def tick(u):
        for n in range(n_head - 1):
            step = u - n

            @pl.when(step == 0)
            def _():
                y_copy(0, 1, shard(n)).wait_recv()
                right_copy(0, n, spot).start()
                left_copy(0, n, spot).start()
                partner_copy(0, n, spot, core).start()

            @pl.when((step >= 1) & (step <= HOPS))
            def _():
                right_copy(step - 1, n, spot - step).wait_recv()

                @pl.when(step < HOPS)
                def _():
                    right_copy(step, n, spot - step).start()

                partner_copy(step, n, spot - step, core).start()
                left_copy(step - 1, n, spot + step).wait_recv()

                @pl.when(step < HOPS)
                def _():
                    left_copy(step, n, spot + step).start()

                partner_copy(HOPS + step, n, spot + step, core).start()

    def ticks(first_tick, last_tick):
        @pl.loop(first_tick, last_tick)
        def _(u):
            tick(u)

    loads[2].wait()
    for what in range(2):
        for k in range(1, n_head):
            bc_copy(k, what, me).start()
        for k in (n_head - 1, 1, 2):
            if what == 0:
                y_copy(0, k, me).start()
        mine = pl.ds(pl.multiple_of(me * piece, piece), piece)
        (bt_ref, ct_ref)[what][mine, :] = (b_ref, c_ref)[what][...]

    for slot in range(1, 4):
        for k in range(1, n_head):
            y_copy(slot, k, me).start()

    n_docs = docs_ref.shape[1]
    lengths = jnp.broadcast_to(docs_ref[...].astype(F32), (n_docs, n_docs))
    up, across = iota((n_docs, n_docs), 0), iota((n_docs, n_docs), 1)
    ends_col = jnp.sum(jnp.where(across <= up, lengths, 0.0), axis=1, keepdims=True)
    lengths_col = jnp.sum(jnp.where(across == up, lengths, 0.0), axis=1, keepdims=True)
    ends_row = jnp.sum(
        jnp.where(up <= across, jnp.broadcast_to(lengths_col, (n_docs, n_docs)), 0.0), axis=0, keepdims=True
    )

    def id_of(position):
        return jnp.sum(jnp.where(position >= ends_row, 1.0, 0.0), axis=1, keepdims=True)

    def ids_of(s):
        start = seq * rows + s * SPAN
        col = id_of((start + iota((SPAN, 1), 0)).astype(F32))
        row = jnp.sum(
            jnp.where((start + iota((1, SPAN), 1)).astype(F32) >= ends_col, 1.0, 0.0), axis=0, keepdims=True
        )
        ahead = start - 1 + iota((1, 1), 0)
        previous = id_of(ahead.astype(F32)) - jnp.where(ahead < 0, 1.0, 0.0)
        last = id_of((start + SPAN - 1 + iota((1, 1), 0)).astype(F32))
        return col, row, previous, last

    spread = (iota((heads, width), 1) // head_size == iota((heads, width), 0)).astype(BF16)
    own_lane = iota((heads, heads), 0) == iota((heads, heads), 1)
    rate = jnp.sum(jnp.where(own_lane, rate_ref[...], 0.0), axis=1, keepdims=True)
    skip = jnp.sum(jnp.where(own_lane, skip_ref[...], 0.0), axis=1, keepdims=True)
    upto = (iota((SPAN, SPAN), 0) <= iota((SPAN, SPAN), 1)).astype(BF16)

    loads[0].wait()

    def scale_span(s, device_decay):
        at = pl.ds(pl.multiple_of(s * SPAN, SPAN), SPAN)
        raw = dt_ref[:, at]
        step = jnp.maximum(raw, 0.0) + jnp.log(1.0 + jnp.exp(-jnp.abs(raw)))
        cum = None
        for term in pieces(-step * rate, 3):
            sums = jnp.dot(term, upto, preferred_element_type=F32)
            cum = sums if cum is None else cum + sums
        middle = 0.5 * cum[:, SPAN - 1 :]
        e_ref[:, at] = jnp.exp(cum - middle)
        forward = step * jnp.exp(middle - cum)
        xf_ref[at, :] = (x_ref[at, :].astype(F32) * expand(forward, spread)).astype(BF16)
        _, _, previous, last = ids_of(s)
        total = jnp.exp(2.0 * middle) * jnp.where(last == previous, 1.0, 0.0)
        both = jnp.where(iota((heads, 16), 1) < 8, jnp.exp(middle), total)
        rows_ref[pl.ds(pl.multiple_of(s * 16, 16), 16), :] = expand(both, spread, 3)
        return device_decay * total

    device_decay = lax.fori_loop(0, spans, scale_span, jnp.ones((heads, 1), F32))
    decay_ref[...] = jnp.zeros_like(decay_ref)
    decay_ref[:, :heads] = jnp.broadcast_to(device_decay, (heads, 128)).T[:8, :]

    def line_peer(k):
        return {"seq": first + (place + k) % line}

    def from_peer(k):
        return (place + line - k) % line

    def decay_copy(k, owner):
        return pltpu.make_async_remote_copy(
            src_ref=decay_ref,
            dst_ref=got_decay.at[owner],
            send_sem=dc_send.at[k],
            recv_sem=dc_recv.at[owner],
            device_id=line_peer(k),
            device_id_type=MESH,
        )

    @pl.loop(1, line)
    def _(k):
        decay_copy(k, place).start()

    got_decay[place] = decay_ref[...]

    for k in range(1, n_head):
        bc_copy(k, 0, (me + n_head - k) % n_head).wait_recv()

    def state_span(s, running):
        at = pl.ds(pl.multiple_of(s * SPAN, SPAN), SPAN)
        before_ref[s] = running
        _, row, _, last = ids_of(s)
        kept = jnp.where(row == last, bt_ref[:, at].astype(F32), 0.0).astype(BF16)
        sums = jnp.dot(kept, xf_ref[at, :], preferred_element_type=F32)
        base = pl.multiple_of(s * 16, 16)
        return rows_ref[pl.ds(base + 8, 1), :] * running + sums * rows_ref[pl.ds(base, 1), :]

    final = lax.fori_loop(0, spans, state_span, jnp.zeros((state_size, width), F32))
    state_ref[...] = final.astype(BF16)

    def own_part(t):
        return (
            pl.ds(pl.multiple_of((t // 2) * part, part), part),
            pl.ds(pl.multiple_of((t % 2) * half, half), half),
        )

    def state_copy(k, owner):
        to = (place + k) % line
        return pltpu.make_async_remote_copy(
            src_ref=state_ref.at[own_part(to)],
            dst_ref=got_state.at[owner],
            send_sem=st_send.at[k],
            recv_sem=st_recv.at[owner],
            device_id=line_peer(k),
            device_id_type=MESH,
        )

    @pl.loop(1, line)
    def _(k):
        state_copy(k, place).start()

    got_state[place] = state_ref[own_part(place)]

    for k in range(1, n_head):
        bc_copy(k, 1, (me + n_head - k) % n_head).wait_recv()
    loads[1].wait()
    skip_row = expand(jnp.broadcast_to(skip, (heads, 8)), spread, 3)[:1, :]

    ticks(0, PLAN[0])

    @pl.loop(0, spans)
    def _(s):
        for i in range(PLAN[1]):
            tick(PLAN[0] + s * PLAN[1] + i)
        at = pl.ds(pl.multiple_of(s * SPAN, SPAN), SPAN)
        col, row, previous, _ = ids_of(s)
        c_here = ct_ref[:, at].T
        scores = jnp.dot(c_here, bt_ref[:, at], preferred_element_type=F32)
        seen = (col == row) & (iota((SPAN, SPAN), 0) >= iota((SPAN, SPAN), 1))
        scores = jnp.where(seen, scores, 0.0).astype(BF16)
        local = jnp.dot(scores, xf_ref[at, :], preferred_element_type=F32)
        inter = jnp.dot(c_here, before_ref[s].astype(BF16), preferred_element_type=F32)
        base = pl.multiple_of(s * 16, 16)
        out_of_middle = expand(e_ref[:, at], spread)
        from_start = rows_ref[pl.ds(base, 1), :] * jnp.where(col == previous, 1.0, 0.0)
        gate = z_ref[at, :].astype(F32)
        gate = gate / (1.0 + jnp.exp(-gate))
        y = out_of_middle * (local + from_start * inter) + skip_row * x_ref[at, :].astype(F32)
        ur_ref[at, :] = y * gate
        as_ref[at, :] = out_of_middle * from_start * gate

    @pl.loop(1, line)
    def _(k):
        decay_copy(k, from_peer(k)).wait_recv()

    @pl.loop(1, line)
    def _(k):
        state_copy(k, from_peer(k)).wait_recv()

    lanes = iota((128, half), 1) + (place % 2) * half
    spread_here = (lanes // head_size == iota((128, half), 0)).astype(BF16)
    decays = expand(got_decay[...].reshape(line * 8, 128).T, spread_here, 3)
    inside, inc = [], jnp.zeros((part, half), F32)
    for d in range(line):
        inside.append(inc)
        inc = decays[8 * d : 8 * d + 1, :] * inc + got_state[d].astype(F32)
    line_ref[...] = inc
    line_copy = pltpu.make_async_remote_copy(
        src_ref=line_ref,
        dst_ref=got_line,
        send_sem=ln_send,
        recv_sem=ln_recv,
        device_id={"seq": (seq + line) % n_seq},
        device_id_type=MESH,
    )
    line_copy.start()
    line_copy.wait_recv()
    factor = jnp.where(at_line + iota((1, half), 0) > 0, 1.0, 0.0)
    earlier = got_line[...]
    for d in range(line):
        back_ref[d] = (inside[d] + factor * earlier).astype(BF16)
        factor = factor * decays[8 * d : 8 * d + 1, :]

    def back_copy(k, owner):
        return pltpu.make_async_remote_copy(
            src_ref=back_ref.at[(place + k) % line],
            dst_ref=inc_ref.at[own_part(owner)],
            send_sem=bk_send.at[k],
            recv_sem=bk_recv.at[owner],
            device_id=line_peer(k),
            device_id_type=MESH,
        )

    @pl.loop(1, line)
    def _(k):
        back_copy(k, place).start()

    inc_ref[own_part(place)] = back_ref[place]

    done = PLAN[0] + spans * PLAN[1]
    ticks(done, done + PLAN[2])
    done += PLAN[2]

    @pl.loop(1, line)
    def _(k):
        back_copy(k, from_peer(k)).wait_recv()

    def finish(block):
        at = pl.ds(pl.multiple_of(block * SPAN, SPAN), SPAN)
        before = jnp.ones((1, width), F32)
        for s in range(spans - 1):
            decay = rows_ref[16 * s + 8 : 16 * s + 9, :]
            before = jnp.where(s + iota((1, width), 0) < block, before * decay, before)
        carried = (inc_ref[...].astype(F32) * before).astype(BF16)
        inter = jnp.dot(ct_ref[:, at].T, carried, preferred_element_type=F32)
        gated = ur_ref[at, :] + as_ref[at, :] * inter
        norm_ref[at, :] = (gated * gain_ref[...]).astype(BF16)
        squares = gated * gated
        folded = squares[:, :128]
        for j in range(1, width // 128):
            folded = folded + squares[:, 128 * j : 128 * (j + 1)]
        row = jnp.sum(folded.T, axis=0, keepdims=True)
        sq_ref[block] = jnp.broadcast_to(row, (8, SPAN))

    def square_copy(k, owner):
        return pltpu.make_async_remote_copy(
            src_ref=sq_ref.at[(me + k) % n_head],
            dst_ref=got_sq.at[owner],
            send_sem=sq_send.at[k],
            recv_sem=sq_recv.at[owner],
            device_id={"head": (me + k) % n_head},
            device_id_type=MESH,
        )

    def rows_of(block, start=0, count=SPAN):
        return norm_ref.at[pl.ds(pl.multiple_of(block * SPAN + start, count), count), :]

    def block_copy(k, owner):
        return pltpu.make_async_remote_copy(
            src_ref=rows_of((me + k) % n_head),
            dst_ref=lhs_ref.at[owner],
            send_sem=a_send.at[k],
            recv_sem=a_recv.at[owner],
            device_id={"head": (me + k) % n_head},
            device_id_type=MESH,
        )

    low = SPAN // 2
    right, left, across_y = (me + 1) % n_head, (me + n_head - 1) % n_head, (me + 2) % n_head

    def relay_copy(way):
        return pltpu.make_async_remote_copy(
            src_ref=rows_of(across_y, way * low, low),
            dst_ref=relay_ref.at[way],
            send_sem=f_send.at[way],
            recv_sem=f_recv.at[way],
            device_id={"head": (right, left)[way]},
            device_id_type=MESH,
        )

    def forward_copy(way, owner):
        return pltpu.make_async_remote_copy(
            src_ref=relay_ref.at[way],
            dst_ref=lhs_ref.at[owner, pl.ds(way * low, low), :],
            send_sem=f_send.at[2 + way],
            recv_sem=f_recv.at[2 + way],
            device_id={"head": (right, left)[way]},
            device_id_type=MESH,
        )

    finish(across_y)
    square_copy(2, me).start()
    relay_copy(0).start()
    relay_copy(1).start()
    finish(right)
    square_copy(1, me).start()
    block_copy(1, me).start()
    finish(left)
    square_copy(n_head - 1, me).start()
    block_copy(n_head - 1, me).start()
    finish(me)
    ticks(done, done + PLAN[3])
    done += PLAN[3]
    relay_copy(0).wait_recv()
    forward_copy(0, left).start()
    relay_copy(1).wait_recv()
    forward_copy(1, right).start()
    ticks(done, HOPS + n_head - 1)

    for slot in range(1, 4):
        for n in range(n_head - 1):
            y_copy(slot, 1, shard(n)).wait_recv()
            partner_copy(2 * HOPS + slot, n, spot + HOPS + slot, core).start()

    cut = 512

    def product(lhs, owner, column):
        return jnp.dot(lhs, wf_ref[owner, :, pl.ds(pl.multiple_of(column, cut), cut)], preferred_element_type=F32)

    def columns(j):
        return pl.ds(pl.multiple_of(j * cut, cut), cut)

    @pl.loop(0, out_width // cut)
    def _(j):
        acc_ref[:, columns(j)] = product(rows_of(me)[...], me, j * cut)

    total = sq_ref[me]
    for k in range(1, n_head):
        owner = (me + n_head - k) % n_head
        square_copy(k, owner).wait_recv()
        total = total + got_sq[owner]
    inverse_rms = lax.rsqrt(total / (width * n_head) + NORM_EPS).T[:, :1]

    def arrived(n):
        @pl.loop(0, CHIPS)
        def _(e):
            place_of = jnp.where(e <= HOPS, other_spot - e, other_spot + e - HOPS)
            partner_copy(e, n, place_of, 1 - core).wait_recv()

    for n in range(2):
        arrived(n)
        block_copy((1, n_head - 1)[n], shard(n)).wait_recv()

        @pl.loop(0, out_width // cut)
        def _(j):
            acc_ref[:, columns(j)] += product(lhs_ref[shard(n)], shard(n), j * cut)

    arrived(2)
    forward_copy(0, across_y).wait_recv()
    forward_copy(1, across_y).wait_recv()

    @pl.loop(0, out_width // cut)
    def _(j):
        own = acc_ref[:, columns(j)] + product(lhs_ref[across_y], across_y, j * cut)
        out_ref[:, columns(j)] = (own * inverse_rms).astype(BF16)

    for k in range(1, n_head):
        for what in range(2):
            bc_copy(k, what, me).wait_send()
        square_copy(k, me).wait_send()

    @pl.loop(1, line)
    def _(k):
        decay_copy(k, place).wait_send()
        state_copy(k, place).wait_send()
        back_copy(k, place).wait_send()

    line_copy.wait_send()
    for slot in range(4):
        for k in range(1, n_head):
            y_copy(slot, k, me).wait_send()
    for way in range(2):
        relay_copy(way).wait_send()
        forward_copy(way, across_y).wait_send()
    block_copy(1, me).wait_send()
    block_copy(n_head - 1, me).wait_send()

    @pl.loop(0, HOPS)
    def _(step):
        for n in range(n_head - 1):
            right_copy(step, n, spot - step).wait_send()
            left_copy(step, n, spot + step).wait_send()

    @pl.loop(0, CHIPS)
    def _(e):
        for n in range(n_head - 1):
            partner_copy(e, n, spot + e, core).wait_send()


def on_device(sizes, x_in, z_gate, b_in, c_in, dt_raw, decay_rate, skip_gain, norm_gain, w_out, doc_lengths):
    n_head, n_seq, line = sizes
    rows, width = x_in.shape
    heads = dt_raw.shape[1]
    out_width = w_out.shape[1]
    state_size = b_in.shape[1] * n_head
    spans = rows // SPAN
    part, half = state_size * 2 // line, width // 2
    vmem, anywhere = pl.BlockSpec(memory_space=pltpu.VMEM), pl.BlockSpec(memory_space=pl.ANY)
    dma = pltpu.SemaphoreType.DMA
    return pl.pallas_call(
        functools.partial(layer_kernel, sizes),
        out_shape=jax.ShapeDtypeStruct((rows // n_head, out_width), BF16),
        in_specs=[vmem] * 7 + [anywhere] * 3,
        out_specs=vmem,
        scratch_shapes=[
            pltpu.VMEM((rows, width), BF16),
            pltpu.VMEM((rows, width), BF16),
            pltpu.VMEM((n_head, *w_out.shape), BF16),
            pltpu.VMEM((state_size, rows), BF16),
            pltpu.VMEM((state_size, rows), BF16),
            pltpu.VMEM((rows, width), BF16),
            pltpu.VMEM((heads, rows), F32),
            pltpu.VMEM((spans * 16, width), F32),
            pltpu.VMEM((spans, state_size, width), F32),
            pltpu.VMEM((rows, width), F32),
            pltpu.VMEM((rows, width), F32),
            pltpu.VMEM((state_size, width), BF16),
            pltpu.VMEM((8, 128), F32),
            pltpu.VMEM((line, part, half), BF16),
            pltpu.VMEM((line, 8, 128), F32),
            pltpu.VMEM((part, half), F32),
            pltpu.VMEM((part, half), F32),
            pltpu.VMEM((line, part, half), BF16),
            pltpu.VMEM((state_size, width), BF16),
            pltpu.VMEM((rows, width), BF16),
            pltpu.VMEM((n_head, 8, SPAN), F32),
            pltpu.VMEM((n_head, 8, SPAN), F32),
            pltpu.VMEM((n_head, rows // n_head, width), BF16),
            pltpu.VMEM((2, rows // n_head // 2, width), BF16),
            pltpu.VMEM((rows // n_head, out_width), F32),
            dma((3,)),
            dma((2, n_head)),
            dma((2, n_head)),
            dma((line,)),
            dma((line,)),
            dma((line,)),
            dma((line,)),
            dma,
            dma,
            dma((line,)),
            dma((line,)),
            dma((n_head,)),
            dma((n_head,)),
            dma((4, n_head)),
            dma((4, n_head)),
            dma((HOPS, n_head - 1)),
            dma((HOPS, n_head - 1)),
            dma((HOPS, n_head - 1)),
            dma((HOPS, n_head - 1)),
            dma((CHIPS, n_head - 1)),
            dma((CHIPS, n_head - 1)),
            dma((n_head,)),
            dma((n_head,)),
            dma((4,)),
            dma((4,)),
        ],
        compiler_params=pltpu.CompilerParams(
            collective_id=0, has_side_effects=True, vmem_limit_bytes=60 * 1024 * 1024
        ),
        name="ssd_layer",
    )(
        b_in.T,
        c_in.T,
        dt_raw.T,
        decay_rate[None, :],
        skip_gain[None, :],
        norm_gain[None, :],
        doc_lengths[None, :],
        x_in,
        z_gate,
        w_out,
    )


def solution(mesh):
    sizes = (mesh.shape["head"], mesh.shape["seq"], 16)
    rows = P("seq", "head")
    return jax.shard_map(
        functools.partial(on_device, sizes),
        mesh=mesh,
        in_specs=(rows, rows, rows, rows, rows, P("head"), P("head"), P("head"), P("head", None), P()),
        out_specs=P(("seq", "head"), None),
        check_vma=False,
    )
```

```python
import functools

import jax
import jax.numpy as jnp
from jax import lax
from jax.experimental import pallas as pl
from jax.experimental.pallas import tpu as pltpu
from jax.sharding import PartitionSpec as P

SPAN = 256
NORM_EPS = 1e-05
MESH = pl.DeviceIdType.MESH
F32 = jnp.float32
BF16 = jnp.bfloat16


SIDES = (1792, 768)
PLAN = (3, 6, 4)
PLANE = (8, 4)
CHIPS = PLANE[0] * PLANE[1]


def gather_steps(core):
    one, two = (0, 1) if core == 0 else (1, 0)

    def moved(by_one, by_two):
        return (by_one, by_two) if core == 0 else (by_two, by_one)

    def hops(axis, opposite):
        size = PLANE[axis]
        rows = []
        for hop in range(1, size // 2 + 1):
            row = []
            for way in range(2):
                if hop < size // 2 or way == opposite:
                    goes_on = hop + 1 < size // 2 or (hop + 1 == size // 2 and way == opposite)
                    row.append((hop if way else -hop, 2 * axis + way, goes_on))
            rows.append(row)
        return rows

    both = [2 * two, 2 * two + 1]
    first = hops(one, 0)
    lines = [(0, 0)] + [(offset, hop + 1) for hop, row in enumerate(first) for offset, _, _ in row]
    steps = []
    for when in range(1, PLANE[one] // 2 + PLANE[two] // 2 + 1):
        if when <= len(first):
            for offset, way, goes_on in first[when - 1]:
                steps.append((*moved(offset, 0), both + ([way] if goes_on else [])))
        for i, (line_offset, ready) in enumerate(lines):
            if 1 <= when - ready <= PLANE[two] // 2:
                for offset, way, goes_on in hops(two, i % 2)[when - ready - 1]:
                    steps.append((*moved(line_offset, offset), [way] if goes_on else []))
    return steps


def pieces(v, terms):
    out = []
    for _ in range(terms):
        part = v.astype(BF16)
        out.append(part)
        v = v - part.astype(F32)
    return out


def expand(v, spread, terms=2):
    total = None
    for part in pieces(v, terms):
        term = lax.dot_general(part, spread, (((0,), (0,)), ((), ())), preferred_element_type=F32)
        total = term if total is None else total + term
    return total


def iota(shape, dim):
    return lax.broadcasted_iota(jnp.int32, shape, dim)


def layer_kernel(
    sizes,
    b_ref, c_ref, dt_ref, rate_ref, skip_ref, gain_ref, docs_ref, x_hbm, z_hbm, w_hbm,
    out_ref,
    x_ref, z_ref, wf_ref, bt_ref, ct_ref, xf_ref, e_ref, rows_ref, before_ref, ur_ref, as_ref,
    state_ref, decay_ref, got_state, got_decay, line_ref, got_line, back_ref, inc_ref, norm_ref,
    sq_ref, got_sq, lhs_ref, relay_ref, acc_ref,
    in_sem, bc_send, bc_recv, st_send, st_recv, dc_send, dc_recv, ln_send, ln_recv, bk_send, bk_recv,
    sq_send, sq_recv, y_send, y_recv, w_send, w_recv, d_send, d_recv,
    a_send, a_recv, f_send, f_recv,
):
    n_head, n_seq, line = sizes
    rows, width = x_ref.shape
    heads = dt_ref.shape[0]
    head_size = width // heads
    state_size = bt_ref.shape[0]
    piece = b_ref.shape[0]
    spans = rows // SPAN
    me, seq = lax.axis_index("head"), lax.axis_index("seq")
    at_line, place = seq // line, seq % line
    first = seq - place
    half = width // 2
    part = state_size * 2 // line

    def load(i, src, dst):
        return pltpu.make_async_copy(src, dst, in_sem.at[i])

    loads = [load(0, x_hbm, x_ref), load(1, z_hbm, z_ref), load(2, w_hbm, wf_ref.at[n_head - 1])]
    for one in loads:
        one.start()

    barrier = pltpu.get_barrier_semaphore()
    for k in range(1, n_head):
        pl.semaphore_signal(barrier, inc=1, device_id={"head": (me + k) % n_head}, device_id_type=MESH)

    @pl.loop(1, line)
    def _(k):
        pl.semaphore_signal(
            barrier, inc=1, device_id={"seq": first + (place + k) % line}, device_id_type=MESH
        )

    for step in (line, n_seq - line):
        pl.semaphore_signal(barrier, inc=1, device_id={"seq": (seq + step) % n_seq}, device_id_type=MESH)
    pl.semaphore_wait(barrier, n_head - 1 + line - 1 + 2)

    def bc_copy(k, what, owner):
        dst = (bt_ref, ct_ref)[what].at[pl.ds(pl.multiple_of(owner * piece, piece), piece), :]
        return pltpu.make_async_remote_copy(
            src_ref=(b_ref, c_ref)[what],
            dst_ref=dst,
            send_sem=bc_send.at[what, k],
            recv_sem=bc_recv.at[what, owner],
            device_id={"head": (me + k) % n_head},
            device_id_type=MESH,
        )

    core = seq % 2
    partner = seq + 1 - 2 * core
    out_width = wf_ref.shape[2]
    slice_rows = wf_ref.shape[1] // CHIPS
    mine_of_w = n_head - 1
    ways = (
        first + (place + 2) % line,
        first + (place + line - 2) % line,
        (seq + line) % n_seq,
        (seq + n_seq - line) % n_seq,
    )

    def chip(along_z, along_x):
        return (at_line + along_x + PLANE[1]) % PLANE[1] * PLANE[0] + (place // 2 + along_z + PLANE[0]) % PLANE[0]

    def shard(n):
        return (me + (1, n_head - 1, 2)[n]) % n_head

    def chunk(of_core, index, who):
        at = pl.multiple_of(who * slice_rows, slice_rows)
        side = pl.ds(0 if of_core == 0 else SIDES[0], SIDES[of_core])
        return wf_ref.at[index, pl.ds(at, slice_rows), side]

    def y_copy(of_core, k, index):
        return pltpu.make_async_remote_copy(
            src_ref=chunk(of_core, mine_of_w, chip(0, 0)),
            dst_ref=chunk(of_core, index, chip(0, 0)),
            send_sem=y_send.at[k],
            recv_sem=y_recv.at[index],
            device_id={"head": (me + k) % n_head},
            device_id_type=MESH,
        )

    def slice_copy(of_core, who, way):
        where = chunk(of_core, pl.ds(0, n_head - 1), who)
        return pltpu.make_async_remote_copy(
            src_ref=where,
            dst_ref=where,
            send_sem=w_send.at[way, who],
            recv_sem=w_recv.at[who],
            device_id={"seq": ways[way]},
            device_id_type=MESH,
        )

    def partner_copy(of_core, who):
        where = chunk(of_core, pl.ds(0, n_head - 1), who)
        return pltpu.make_async_remote_copy(
            src_ref=where,
            dst_ref=where,
            send_sem=d_send.at[who],
            recv_sem=d_recv.at[who],
            device_id={"seq": partner},
            device_id_type=MESH,
        )

    def on_each_core(what):
        for of_core in range(2):
            pl.when(core == of_core)(functools.partial(what, of_core))

    def start_gather(of_core):
        for n in range(n_head - 1):
            y_copy(of_core, 1, n).wait_recv()
        for way in range(4):
            slice_copy(of_core, chip(0, 0), way).start()
        partner_copy(of_core, chip(0, 0)).start()

    def gather(first_step, last_step):
        def run(of_core):
            for along_z, along_x, on in gather_steps(of_core)[first_step:last_step]:
                who = chip(along_z, along_x)
                slice_copy(of_core, who, 0).wait_recv()
                for way in on:
                    slice_copy(of_core, who, way).start()
                partner_copy(of_core, who).start()

        on_each_core(run)

    def start_y(of_core):
        for k, index in ((1, 1), (n_head - 1, 0), (2, 2)):
            y_copy(of_core, k, index).start()

    loads[2].wait()
    for what in range(2):
        for k in range(1, n_head):
            bc_copy(k, what, me).start()
        if what == 0:
            on_each_core(start_y)
        mine = pl.ds(pl.multiple_of(me * piece, piece), piece)
        (bt_ref, ct_ref)[what][mine, :] = (b_ref, c_ref)[what][...]

    n_docs = docs_ref.shape[1]
    lengths = jnp.broadcast_to(docs_ref[...].astype(F32), (n_docs, n_docs))
    up, across = iota((n_docs, n_docs), 0), iota((n_docs, n_docs), 1)
    ends_col = jnp.sum(jnp.where(across <= up, lengths, 0.0), axis=1, keepdims=True)
    lengths_col = jnp.sum(jnp.where(across == up, lengths, 0.0), axis=1, keepdims=True)
    ends_row = jnp.sum(
        jnp.where(up <= across, jnp.broadcast_to(lengths_col, (n_docs, n_docs)), 0.0), axis=0, keepdims=True
    )

    def id_of(position):
        return jnp.sum(jnp.where(position >= ends_row, 1.0, 0.0), axis=1, keepdims=True)

    def ids_of(s):
        start = seq * rows + s * SPAN
        col = id_of((start + iota((SPAN, 1), 0)).astype(F32))
        row = jnp.sum(
            jnp.where((start + iota((1, SPAN), 1)).astype(F32) >= ends_col, 1.0, 0.0), axis=0, keepdims=True
        )
        ahead = start - 1 + iota((1, 1), 0)
        previous = id_of(ahead.astype(F32)) - jnp.where(ahead < 0, 1.0, 0.0)
        last = id_of((start + SPAN - 1 + iota((1, 1), 0)).astype(F32))
        return col, row, previous, last

    spread = (iota((heads, width), 1) // head_size == iota((heads, width), 0)).astype(BF16)
    own_lane = iota((heads, heads), 0) == iota((heads, heads), 1)
    rate = jnp.sum(jnp.where(own_lane, rate_ref[...], 0.0), axis=1, keepdims=True)
    skip = jnp.sum(jnp.where(own_lane, skip_ref[...], 0.0), axis=1, keepdims=True)
    upto = (iota((SPAN, SPAN), 0) <= iota((SPAN, SPAN), 1)).astype(BF16)

    loads[0].wait()

    def scale_span(s, device_decay):
        at = pl.ds(pl.multiple_of(s * SPAN, SPAN), SPAN)
        raw = dt_ref[:, at]
        step = jnp.maximum(raw, 0.0) + jnp.log(1.0 + jnp.exp(-jnp.abs(raw)))
        cum = None
        for term in pieces(-step * rate, 3):
            sums = jnp.dot(term, upto, preferred_element_type=F32)
            cum = sums if cum is None else cum + sums
        middle = 0.5 * cum[:, SPAN - 1 :]
        e_ref[:, at] = jnp.exp(cum - middle)
        forward = step * jnp.exp(middle - cum)
        xf_ref[at, :] = (x_ref[at, :].astype(F32) * expand(forward, spread)).astype(BF16)
        _, _, previous, last = ids_of(s)
        total = jnp.exp(2.0 * middle) * jnp.where(last == previous, 1.0, 0.0)
        both = jnp.where(iota((heads, 16), 1) < 8, jnp.exp(middle), total)
        rows_ref[pl.ds(pl.multiple_of(s * 16, 16), 16), :] = expand(both, spread, 3)
        return device_decay * total

    device_decay = lax.fori_loop(0, spans, scale_span, jnp.ones((heads, 1), F32))
    decay_ref[...] = jnp.zeros_like(decay_ref)
    decay_ref[:, :heads] = jnp.broadcast_to(device_decay, (heads, 128)).T[:8, :]

    def line_peer(k):
        return {"seq": first + (place + k) % line}

    def from_peer(k):
        return (place + line - k) % line

    def decay_copy(k, owner):
        return pltpu.make_async_remote_copy(
            src_ref=decay_ref,
            dst_ref=got_decay.at[owner],
            send_sem=dc_send.at[k],
            recv_sem=dc_recv.at[owner],
            device_id=line_peer(k),
            device_id_type=MESH,
        )

    @pl.loop(1, line)
    def _(k):
        decay_copy(k, place).start()

    got_decay[place] = decay_ref[...]

    for k in range(1, n_head):
        bc_copy(k, 0, (me + n_head - k) % n_head).wait_recv()

    def state_span(s, running):
        at = pl.ds(pl.multiple_of(s * SPAN, SPAN), SPAN)
        before_ref[s] = running
        _, row, _, last = ids_of(s)
        kept = jnp.where(row == last, bt_ref[:, at].astype(F32), 0.0).astype(BF16)
        sums = jnp.dot(kept, xf_ref[at, :], preferred_element_type=F32)
        base = pl.multiple_of(s * 16, 16)
        return rows_ref[pl.ds(base + 8, 1), :] * running + sums * rows_ref[pl.ds(base, 1), :]

    final = lax.fori_loop(0, spans, state_span, jnp.zeros((state_size, width), F32))
    state_ref[...] = final.astype(BF16)

    def own_part(t):
        return (
            pl.ds(pl.multiple_of((t // 2) * part, part), part),
            pl.ds(pl.multiple_of((t % 2) * half, half), half),
        )

    def state_copy(k, owner):
        to = (place + k) % line
        return pltpu.make_async_remote_copy(
            src_ref=state_ref.at[own_part(to)],
            dst_ref=got_state.at[owner],
            send_sem=st_send.at[k],
            recv_sem=st_recv.at[owner],
            device_id=line_peer(k),
            device_id_type=MESH,
        )

    @pl.loop(1, line)
    def _(k):
        state_copy(k, place).start()

    got_state[place] = state_ref[own_part(place)]

    for k in range(1, n_head):
        bc_copy(k, 1, (me + n_head - k) % n_head).wait_recv()
    loads[1].wait()
    skip_row = expand(jnp.broadcast_to(skip, (heads, 8)), spread, 3)[:1, :]

    on_each_core(start_gather)

    @pl.loop(0, spans)
    def _(s):
        at = pl.ds(pl.multiple_of(s * SPAN, SPAN), SPAN)
        col, row, previous, _ = ids_of(s)
        c_here = ct_ref[:, at].T
        scores = jnp.dot(c_here, bt_ref[:, at], preferred_element_type=F32)
        seen = (col == row) & (iota((SPAN, SPAN), 0) >= iota((SPAN, SPAN), 1))
        scores = jnp.where(seen, scores, 0.0).astype(BF16)
        local = jnp.dot(scores, xf_ref[at, :], preferred_element_type=F32)
        inter = jnp.dot(c_here, before_ref[s].astype(BF16), preferred_element_type=F32)
        base = pl.multiple_of(s * 16, 16)
        out_of_middle = expand(e_ref[:, at], spread)
        from_start = rows_ref[pl.ds(base, 1), :] * jnp.where(col == previous, 1.0, 0.0)
        gate = z_ref[at, :].astype(F32)
        gate = gate / (1.0 + jnp.exp(-gate))
        y = out_of_middle * (local + from_start * inter) + skip_row * x_ref[at, :].astype(F32)
        ur_ref[at, :] = y * gate
        as_ref[at, :] = out_of_middle * from_start * gate

    gather(0, PLAN[0])

    @pl.loop(1, line)
    def _(k):
        decay_copy(k, from_peer(k)).wait_recv()

    @pl.loop(1, line)
    def _(k):
        state_copy(k, from_peer(k)).wait_recv()

    lanes = iota((128, half), 1) + (place % 2) * half
    spread_here = (lanes // head_size == iota((128, half), 0)).astype(BF16)
    decays = expand(got_decay[...].reshape(line * 8, 128).T, spread_here, 3)
    inside, inc = [], jnp.zeros((part, half), F32)
    for d in range(line):
        inside.append(inc)
        inc = decays[8 * d : 8 * d + 1, :] * inc + got_state[d].astype(F32)
    line_ref[...] = inc
    line_copy = pltpu.make_async_remote_copy(
        src_ref=line_ref,
        dst_ref=got_line,
        send_sem=ln_send,
        recv_sem=ln_recv,
        device_id={"seq": (seq + line) % n_seq},
        device_id_type=MESH,
    )
    line_copy.start()
    line_copy.wait_recv()
    factor = jnp.where(at_line + iota((1, half), 0) > 0, 1.0, 0.0)
    earlier = got_line[...]
    for d in range(line):
        back_ref[d] = (inside[d] + factor * earlier).astype(BF16)
        factor = factor * decays[8 * d : 8 * d + 1, :]

    def back_copy(k, owner):
        return pltpu.make_async_remote_copy(
            src_ref=back_ref.at[(place + k) % line],
            dst_ref=inc_ref.at[own_part(owner)],
            send_sem=bk_send.at[k],
            recv_sem=bk_recv.at[owner],
            device_id=line_peer(k),
            device_id_type=MESH,
        )

    @pl.loop(1, line)
    def _(k):
        back_copy(k, place).start()

    inc_ref[own_part(place)] = back_ref[place]

    gather(PLAN[0], PLAN[0] + PLAN[1])

    @pl.loop(1, line)
    def _(k):
        back_copy(k, from_peer(k)).wait_recv()

    def finish(block):
        at = pl.ds(pl.multiple_of(block * SPAN, SPAN), SPAN)
        before = jnp.ones((1, width), F32)
        for s in range(spans - 1):
            decay = rows_ref[16 * s + 8 : 16 * s + 9, :]
            before = jnp.where(s + iota((1, width), 0) < block, before * decay, before)
        carried = (inc_ref[...].astype(F32) * before).astype(BF16)
        inter = jnp.dot(ct_ref[:, at].T, carried, preferred_element_type=F32)
        gated = ur_ref[at, :] + as_ref[at, :] * inter
        norm_ref[at, :] = (gated * gain_ref[...]).astype(BF16)
        squares = gated * gated
        folded = squares[:, :128]
        for j in range(1, width // 128):
            folded = folded + squares[:, 128 * j : 128 * (j + 1)]
        row = jnp.sum(folded.T, axis=0, keepdims=True)
        sq_ref[block] = jnp.broadcast_to(row, (8, SPAN))

    def square_copy(k, owner):
        return pltpu.make_async_remote_copy(
            src_ref=sq_ref.at[(me + k) % n_head],
            dst_ref=got_sq.at[owner],
            send_sem=sq_send.at[k],
            recv_sem=sq_recv.at[owner],
            device_id={"head": (me + k) % n_head},
            device_id_type=MESH,
        )

    def rows_of(block, start=0, count=SPAN):
        return norm_ref.at[pl.ds(pl.multiple_of(block * SPAN + start, count), count), :]

    def block_copy(k, owner):
        return pltpu.make_async_remote_copy(
            src_ref=rows_of((me + k) % n_head),
            dst_ref=lhs_ref.at[owner],
            send_sem=a_send.at[k],
            recv_sem=a_recv.at[owner],
            device_id={"head": (me + k) % n_head},
            device_id_type=MESH,
        )

    low = SPAN // 2
    right, left, across_y = (me + 1) % n_head, (me + n_head - 1) % n_head, (me + 2) % n_head

    def relay_copy(way):
        return pltpu.make_async_remote_copy(
            src_ref=rows_of(across_y, way * low, low),
            dst_ref=relay_ref.at[way],
            send_sem=f_send.at[way],
            recv_sem=f_recv.at[way],
            device_id={"head": (right, left)[way]},
            device_id_type=MESH,
        )

    def forward_copy(way, owner):
        return pltpu.make_async_remote_copy(
            src_ref=relay_ref.at[way],
            dst_ref=lhs_ref.at[owner, pl.ds(way * low, low), :],
            send_sem=f_send.at[2 + way],
            recv_sem=f_recv.at[2 + way],
            device_id={"head": (right, left)[way]},
            device_id_type=MESH,
        )

    finish(across_y)
    square_copy(2, me).start()
    relay_copy(0).start()
    relay_copy(1).start()
    finish(right)
    square_copy(1, me).start()
    block_copy(1, me).start()
    finish(left)
    square_copy(n_head - 1, me).start()
    block_copy(n_head - 1, me).start()
    finish(me)
    gather(PLAN[0] + PLAN[1], sum(PLAN))
    relay_copy(0).wait_recv()
    forward_copy(0, left).start()
    relay_copy(1).wait_recv()
    forward_copy(1, right).start()
    gather(sum(PLAN), CHIPS)

    cut = 512

    def product(lhs, owner, column):
        return jnp.dot(lhs, wf_ref[owner, :, pl.ds(pl.multiple_of(column, cut), cut)], preferred_element_type=F32)

    def columns(j):
        return pl.ds(pl.multiple_of(j * cut, cut), cut)

    @pl.loop(0, out_width // cut)
    def _(j):
        acc_ref[:, columns(j)] = product(rows_of(me)[...], mine_of_w, j * cut)

    total = sq_ref[me]
    for k in range(1, n_head):
        owner = (me + n_head - k) % n_head
        square_copy(k, owner).wait_recv()
        total = total + got_sq[owner]
    inverse_rms = lax.rsqrt(total / (width * n_head) + NORM_EPS).T[:, :1]

    def other_half(of_core):
        @pl.loop(0, CHIPS)
        def _(who):
            partner_copy(1 - of_core, who).wait_recv()

    on_each_core(other_half)
    for n in range(2):
        block_copy((1, n_head - 1)[n], shard(n)).wait_recv()

        @pl.loop(0, out_width // cut)
        def _(j):
            acc_ref[:, columns(j)] += product(lhs_ref[shard(n)], n, j * cut)

    forward_copy(0, across_y).wait_recv()
    forward_copy(1, across_y).wait_recv()

    @pl.loop(0, out_width // cut)
    def _(j):
        own = acc_ref[:, columns(j)] + product(lhs_ref[across_y], 2, j * cut)
        out_ref[:, columns(j)] = (own * inverse_rms).astype(BF16)

    for k in range(1, n_head):
        for what in range(2):
            bc_copy(k, what, me).wait_send()
        square_copy(k, me).wait_send()

    @pl.loop(1, line)
    def _(k):
        decay_copy(k, place).wait_send()
        state_copy(k, place).wait_send()
        back_copy(k, place).wait_send()

    line_copy.wait_send()
    for way in range(2):
        relay_copy(way).wait_send()
        forward_copy(way, across_y).wait_send()
    block_copy(1, me).wait_send()
    block_copy(n_head - 1, me).wait_send()

    def all_left(of_core):
        for k in range(1, n_head):
            y_copy(of_core, k, 0).wait_send()
        for way in range(4):
            slice_copy(of_core, chip(0, 0), way).wait_send()
        for along_z, along_x, on in gather_steps(of_core):
            for way in on:
                slice_copy(of_core, chip(along_z, along_x), way).wait_send()

        @pl.loop(0, CHIPS)
        def _(who):
            partner_copy(of_core, who).wait_send()

    on_each_core(all_left)


def on_device(sizes, x_in, z_gate, b_in, c_in, dt_raw, decay_rate, skip_gain, norm_gain, w_out, doc_lengths):
    n_head, n_seq, line = sizes
    rows, width = x_in.shape
    heads = dt_raw.shape[1]
    out_width = w_out.shape[1]
    state_size = b_in.shape[1] * n_head
    spans = rows // SPAN
    part, half = state_size * 2 // line, width // 2
    vmem, anywhere = pl.BlockSpec(memory_space=pltpu.VMEM), pl.BlockSpec(memory_space=pl.ANY)
    dma = pltpu.SemaphoreType.DMA
    return pl.pallas_call(
        functools.partial(layer_kernel, sizes),
        out_shape=jax.ShapeDtypeStruct((rows // n_head, out_width), BF16),
        in_specs=[vmem] * 7 + [anywhere] * 3,
        out_specs=vmem,
        scratch_shapes=[
            pltpu.VMEM((rows, width), BF16),
            pltpu.VMEM((rows, width), BF16),
            pltpu.VMEM((n_head, *w_out.shape), BF16),
            pltpu.VMEM((state_size, rows), BF16),
            pltpu.VMEM((state_size, rows), BF16),
            pltpu.VMEM((rows, width), BF16),
            pltpu.VMEM((heads, rows), F32),
            pltpu.VMEM((spans * 16, width), F32),
            pltpu.VMEM((spans, state_size, width), F32),
            pltpu.VMEM((rows, width), F32),
            pltpu.VMEM((rows, width), F32),
            pltpu.VMEM((state_size, width), BF16),
            pltpu.VMEM((8, 128), F32),
            pltpu.VMEM((line, part, half), BF16),
            pltpu.VMEM((line, 8, 128), F32),
            pltpu.VMEM((part, half), F32),
            pltpu.VMEM((part, half), F32),
            pltpu.VMEM((line, part, half), BF16),
            pltpu.VMEM((state_size, width), BF16),
            pltpu.VMEM((rows, width), BF16),
            pltpu.VMEM((n_head, 8, SPAN), F32),
            pltpu.VMEM((n_head, 8, SPAN), F32),
            pltpu.VMEM((n_head, rows // n_head, width), BF16),
            pltpu.VMEM((2, rows // n_head // 2, width), BF16),
            pltpu.VMEM((rows // n_head, out_width), F32),
            dma((3,)),
            dma((2, n_head)),
            dma((2, n_head)),
            dma((line,)),
            dma((line,)),
            dma((line,)),
            dma((line,)),
            dma,
            dma,
            dma((line,)),
            dma((line,)),
            dma((n_head,)),
            dma((n_head,)),
            dma((n_head,)),
            dma((n_head,)),
            dma((4, CHIPS)),
            dma((CHIPS,)),
            dma((CHIPS,)),
            dma((CHIPS,)),
            dma((n_head,)),
            dma((n_head,)),
            dma((4,)),
            dma((4,)),
        ],
        compiler_params=pltpu.CompilerParams(
            collective_id=0, has_side_effects=True, vmem_limit_bytes=60 * 1024 * 1024
        ),
        name="ssd_layer",
    )(
        b_in.T,
        c_in.T,
        dt_raw.T,
        decay_rate[None, :],
        skip_gain[None, :],
        norm_gain[None, :],
        doc_lengths[None, :],
        x_in,
        z_gate,
        w_out,
    )


def solution(mesh):
    sizes = (mesh.shape["head"], mesh.shape["seq"], 16)
    rows = P("seq", "head")
    return jax.shard_map(
        functools.partial(on_device, sizes),
        mesh=mesh,
        in_specs=(rows, rows, rows, rows, rows, P("head"), P("head"), P("head"), P("head", None), P()),
        out_specs=P(("seq", "head"), None),
        check_vma=False,
    )
```

```python
import functools

import jax
import jax.numpy as jnp
from jax import lax
from jax.experimental import pallas as pl
from jax.experimental.pallas import tpu as pltpu
from jax.sharding import PartitionSpec as P

SPAN = 256
NORM_EPS = 1e-05
MESH = pl.DeviceIdType.MESH
F32 = jnp.float32
BF16 = jnp.bfloat16


def pieces(v, terms):
    out = []
    for _ in range(terms):
        part = v.astype(BF16)
        out.append(part)
        v = v - part.astype(F32)
    return out


def expand(v, spread, terms=2):
    total = None
    for part in pieces(v, terms):
        term = lax.dot_general(part, spread, (((0,), (0,)), ((), ())), preferred_element_type=F32)
        total = term if total is None else total + term
    return total


def iota(shape, dim):
    return lax.broadcasted_iota(jnp.int32, shape, dim)


def layer_kernel(
    sizes,
    b_hbm, c_hbm, dt_hbm, rate_hbm, skip_hbm, gain_hbm, docs_hbm, x_hbm, z_hbm, w_hbm,
    out_ref,
    b_ref, c_ref, dt_ref, rate_ref, skip_ref, gain_ref, docs_ref, x_ref, z_ref, w_ref, bt_ref, ct_ref, xf_ref, e_ref, rows_ref, before_ref, ur_ref, as_ref,
    state_ref, decay_ref, got_state, got_decay, line_ref, got_line, back_ref, inc_ref, norm_ref,
    sq_ref, got_sq, send_r, got_r, send_l, got_l, decays_ref,
    in_sem, bc_send, bc_recv, st_send, st_recv, dc_send, dc_recv, ln_send, ln_recv, bk_send, bk_recv,
    sq_send, sq_recv, r_send, r_recv, l_send, l_recv,
):
    n_head, n_seq, line = sizes
    rows, width = x_ref.shape
    heads = dt_ref.shape[0]
    head_size = width // heads
    state_size = bt_ref.shape[0]
    piece = b_ref.shape[0]
    spans = rows // SPAN
    me, seq = lax.axis_index("head"), lax.axis_index("seq")
    at_line, place = seq // line, seq % line
    first = seq - place
    half = width // 2
    part = state_size * 2 // line

    def load(i, src, dst):
        return pltpu.make_async_copy(src, dst, in_sem.at[i])

    barrier = pltpu.get_barrier_semaphore()
    for k in range(1, n_head):
        pl.semaphore_signal(barrier, inc=1, device_id={"head": (me + k) % n_head}, device_id_type=MESH)

    @pl.loop(1, line)
    def _(k):
        pl.semaphore_signal(
            barrier, inc=1, device_id={"seq": first + (place + k) % line}, device_id_type=MESH
        )

    for step in (line, n_seq - line):
        pl.semaphore_signal(barrier, inc=1, device_id={"seq": (seq + step) % n_seq}, device_id_type=MESH)
    sources = (b_hbm, dt_hbm, rate_hbm, docs_hbm, x_hbm, c_hbm, skip_hbm, gain_hbm, z_hbm, w_hbm)
    targets = (b_ref, dt_ref, rate_ref, docs_ref, x_ref, c_ref, skip_ref, gain_ref, z_ref, w_ref)
    loads = [load(i, *pair) for i, pair in enumerate(zip(sources, targets))]
    for one in loads:
        one.start()
    for one in loads[:4]:
        one.wait()
    loads[5].wait()
    pl.semaphore_wait(barrier, n_head - 1 + line - 1 + 2)

    def bc_copy(k, what, owner):
        dst = (bt_ref, ct_ref)[what].at[pl.ds(pl.multiple_of(owner * piece, piece), piece), :]
        return pltpu.make_async_remote_copy(
            src_ref=(b_ref, c_ref)[what],
            dst_ref=dst,
            send_sem=bc_send.at[what, k],
            recv_sem=bc_recv.at[what, owner],
            device_id={"head": (me + k) % n_head},
            device_id_type=MESH,
        )

    for what in range(2):
        for k in range(1, n_head):
            bc_copy(k, what, me).start()
        mine = pl.ds(pl.multiple_of(me * piece, piece), piece)
        (bt_ref, ct_ref)[what][mine, :] = (b_ref, c_ref)[what][...]

    n_docs = docs_ref.shape[1]
    lengths = jnp.broadcast_to(docs_ref[...].astype(F32), (n_docs, n_docs))
    up, across = iota((n_docs, n_docs), 0), iota((n_docs, n_docs), 1)
    ends_col = jnp.sum(jnp.where(across <= up, lengths, 0.0), axis=1, keepdims=True)
    lengths_col = jnp.sum(jnp.where(across == up, lengths, 0.0), axis=1, keepdims=True)
    ends_row = jnp.sum(
        jnp.where(up <= across, jnp.broadcast_to(lengths_col, (n_docs, n_docs)), 0.0), axis=0, keepdims=True
    )

    def id_of(position):
        return jnp.sum(jnp.where(position >= ends_row, 1.0, 0.0), axis=1, keepdims=True)

    def ids_of(s):
        start = seq * rows + s * SPAN
        col = id_of((start + iota((SPAN, 1), 0)).astype(F32))
        row = jnp.sum(
            jnp.where((start + iota((1, SPAN), 1)).astype(F32) >= ends_col, 1.0, 0.0), axis=0, keepdims=True
        )
        ahead = start - 1 + iota((1, 1), 0)
        previous = id_of(ahead.astype(F32)) - jnp.where(ahead < 0, 1.0, 0.0)
        last = id_of((start + SPAN - 1 + iota((1, 1), 0)).astype(F32))
        return col, row, previous, last

    spread = (iota((heads, width), 1) // head_size == iota((heads, width), 0)).astype(BF16)
    own_lane = iota((heads, heads), 0) == iota((heads, heads), 1)
    rate = jnp.sum(jnp.where(own_lane, rate_ref[...], 0.0), axis=1, keepdims=True)
    upto = (iota((SPAN, SPAN), 0) <= iota((SPAN, SPAN), 1)).astype(BF16)

    loads[4].wait()

    def scale_span(s, device_decay):
        at = pl.ds(pl.multiple_of(s * SPAN, SPAN), SPAN)
        raw = dt_ref[:, at]
        step = jnp.maximum(raw, 0.0) + jnp.log(1.0 + jnp.exp(-jnp.abs(raw)))
        cum = None
        for term in pieces(-step * rate, 3):
            sums = jnp.dot(term, upto, preferred_element_type=F32)
            cum = sums if cum is None else cum + sums
        middle = 0.5 * cum[:, SPAN - 1 :]
        e_ref[:, at] = jnp.exp(cum - middle)
        forward = step * jnp.exp(middle - cum)
        xf_ref[at, :] = (x_ref[at, :].astype(F32) * expand(forward, spread)).astype(BF16)
        _, _, previous, last = ids_of(s)
        total = jnp.exp(2.0 * middle) * jnp.where(last == previous, 1.0, 0.0)
        both = jnp.where(iota((heads, 16), 1) < 8, jnp.exp(middle), total)
        rows_ref[pl.ds(pl.multiple_of(s * 16, 16), 16), :] = expand(both, spread, 3)
        return device_decay * total

    device_decay = lax.fori_loop(0, spans, scale_span, jnp.ones((heads, 1), F32))
    decay_ref[...] = jnp.zeros_like(decay_ref)
    decay_ref[:, :heads] = jnp.broadcast_to(device_decay, (heads, 128)).T[:8, :]

    def line_peer(k):
        return {"seq": first + (place + k) % line}

    def from_peer(k):
        return (place + line - k) % line

    def decay_copy(k, owner):
        return pltpu.make_async_remote_copy(
            src_ref=decay_ref,
            dst_ref=got_decay.at[owner],
            send_sem=dc_send.at[k],
            recv_sem=dc_recv.at[owner],
            device_id=line_peer(k),
            device_id_type=MESH,
        )

    @pl.loop(1, line)
    def _(k):
        decay_copy(k, place).start()

    got_decay[place] = decay_ref[...]

    for k in range(1, n_head):
        bc_copy(k, 0, (me + n_head - k) % n_head).wait_recv()

    def state_span(s, running):
        at = pl.ds(pl.multiple_of(s * SPAN, SPAN), SPAN)
        before_ref[s] = running
        _, row, _, last = ids_of(s)
        kept = jnp.where(row == last, bt_ref[:, at].astype(F32), 0.0).astype(BF16)
        sums = jnp.dot(kept, xf_ref[at, :], preferred_element_type=F32)
        base = pl.multiple_of(s * 16, 16)
        return rows_ref[pl.ds(base + 8, 1), :] * running + sums * rows_ref[pl.ds(base, 1), :]

    final = lax.fori_loop(0, spans, state_span, jnp.zeros((state_size, width), F32))
    state_ref[...] = final.astype(BF16)

    def own_part(t):
        return (
            pl.ds(pl.multiple_of((t // 2) * part, part), part),
            pl.ds(pl.multiple_of((t % 2) * half, half), half),
        )

    def state_copy(k, owner):
        to = (place + k) % line
        return pltpu.make_async_remote_copy(
            src_ref=state_ref.at[own_part(to)],
            dst_ref=got_state.at[owner],
            send_sem=st_send.at[k],
            recv_sem=st_recv.at[owner],
            device_id=line_peer(k),
            device_id_type=MESH,
        )

    @pl.loop(1, line)
    def _(k):
        state_copy(k, place).start()

    got_state[place] = state_ref[own_part(place)]

    @pl.loop(1, line)
    def _(k):
        decay_copy(k, from_peer(k)).wait_recv()

    lanes = iota((128, half), 1) + (place % 2) * half
    spread_here = (lanes // head_size == iota((128, half), 0)).astype(BF16)
    decays_ref[...] = expand(got_decay[...].reshape(line * 8, 128).T, spread_here, 3)
    for k in range(1, n_head):
        bc_copy(k, 1, (me + n_head - k) % n_head).wait_recv()
    for one in loads[6:9]:
        one.wait()
    skip = jnp.sum(jnp.where(own_lane, skip_ref[...], 0.0), axis=1, keepdims=True)
    skip_row = expand(jnp.broadcast_to(skip, (heads, 8)), spread, 3)[:1, :]

    @pl.loop(0, spans)
    def _(s):
        at = pl.ds(pl.multiple_of(s * SPAN, SPAN), SPAN)
        col, row, previous, _ = ids_of(s)
        c_here = ct_ref[:, at].T
        scores = jnp.dot(c_here, bt_ref[:, at], preferred_element_type=F32)
        seen = (col == row) & (iota((SPAN, SPAN), 0) >= iota((SPAN, SPAN), 1))
        scores = jnp.where(seen, scores, 0.0).astype(BF16)
        local = jnp.dot(scores, xf_ref[at, :], preferred_element_type=F32)
        inter = jnp.dot(c_here, before_ref[s].astype(BF16), preferred_element_type=F32)
        base = pl.multiple_of(s * 16, 16)
        out_of_middle = expand(e_ref[:, at], spread)
        from_start = rows_ref[pl.ds(base, 1), :] * jnp.where(col == previous, 1.0, 0.0)
        gate = z_ref[at, :].astype(F32)
        gate = gate / (1.0 + jnp.exp(-gate))
        y = out_of_middle * (local + from_start * inter) + skip_row * x_ref[at, :].astype(F32)
        ur_ref[at, :] = y * gate
        as_ref[at, :] = out_of_middle * from_start * gate

    @pl.loop(1, line)
    def _(k):
        state_copy(k, from_peer(k)).wait_recv()

    inside, inc = [], jnp.zeros((part, half), F32)
    for d in range(line):
        inside.append(inc)
        inc = decays_ref[8 * d : 8 * d + 1, :] * inc + got_state[d].astype(F32)
    line_ref[...] = inc
    line_copy = pltpu.make_async_remote_copy(
        src_ref=line_ref,
        dst_ref=got_line,
        send_sem=ln_send,
        recv_sem=ln_recv,
        device_id={"seq": (seq + line) % n_seq},
        device_id_type=MESH,
    )
    line_copy.start()
    line_copy.wait_recv()
    factor = jnp.where(at_line + iota((1, half), 0) > 0, 1.0, 0.0)
    earlier = got_line[...]
    for d in range(line):
        back_ref[d] = (inside[d] + factor * earlier).astype(BF16)
        factor = factor * decays_ref[8 * d : 8 * d + 1, :]

    def back_copy(k, owner):
        return pltpu.make_async_remote_copy(
            src_ref=back_ref.at[(place + k) % line],
            dst_ref=inc_ref.at[own_part(owner)],
            send_sem=bk_send.at[k],
            recv_sem=bk_recv.at[owner],
            device_id=line_peer(k),
            device_id_type=MESH,
        )

    @pl.loop(1, line)
    def _(k):
        back_copy(k, place).start()

    inc_ref[own_part(place)] = back_ref[place]

    loads[9].wait()

    @pl.loop(1, line)
    def _(k):
        back_copy(k, from_peer(k)).wait_recv()

    def finish(block):
        at = pl.ds(pl.multiple_of(block * SPAN, SPAN), SPAN)
        before = jnp.ones((1, width), F32)
        for s in range(spans - 1):
            decay = rows_ref[16 * s + 8 : 16 * s + 9, :]
            before = jnp.where(s + iota((1, width), 0) < block, before * decay, before)
        carried = (inc_ref[...].astype(F32) * before).astype(BF16)
        inter = jnp.dot(ct_ref[:, at].T, carried, preferred_element_type=F32)
        gated = ur_ref[at, :] + as_ref[at, :] * inter
        norm_ref[at, :] = (gated * gain_ref[...]).astype(BF16)
        squares = gated * gated
        folded = squares[:, :128]
        for j in range(1, width // 128):
            folded = folded + squares[:, 128 * j : 128 * (j + 1)]
        row = jnp.sum(folded.T, axis=0, keepdims=True)
        sq_ref[block] = jnp.broadcast_to(row, (8, SPAN))

    def square_copy(k, owner):
        return pltpu.make_async_remote_copy(
            src_ref=sq_ref.at[(me + k) % n_head],
            dst_ref=got_sq.at[owner],
            send_sem=sq_send.at[k],
            recv_sem=sq_recv.at[owner],
            device_id={"head": (me + k) % n_head},
            device_id_type=MESH,
        )

    out_width = out_ref.shape[1]
    parts, cut = got_r.shape[1], got_r.shape[3]

    def product(block, column):
        return jnp.dot(
            norm_ref[pl.ds(pl.multiple_of(block * SPAN, SPAN), SPAN), :],
            w_ref[:, pl.ds(pl.multiple_of(column, cut), cut)],
            preferred_element_type=F32,
        )

    def right_copy(step, j):
        return pltpu.make_async_remote_copy(
            src_ref=send_r.at[step, j],
            dst_ref=got_r.at[step, j],
            send_sem=r_send.at[step, j],
            recv_sem=r_recv.at[step, j],
            device_id={"head": (me + 1) % n_head},
            device_id_type=MESH,
        )

    def left_copy(step, j):
        return pltpu.make_async_remote_copy(
            src_ref=send_l.at[step, j],
            dst_ref=got_l.at[step, j],
            send_sem=l_send.at[step, j],
            recv_sem=l_recv.at[step, j],
            device_id={"head": (me + n_head - 1) % n_head},
            device_id_type=MESH,
        )

    ahead, behind = (me + n_head - 1) % n_head, (me + 1) % n_head
    def first_right(j):
        send_r[0, j] = product(ahead, j * cut).astype(BF16)
        right_copy(0, j).start()

    def first_left(j):
        send_l[0, j] = product(behind, out_width // 2 + j * cut).astype(BF16)
        left_copy(0, j).start()

    finish(ahead)
    first_right(0)
    finish(behind)
    first_left(0)

    @pl.loop(1, parts)
    def _(j):
        first_right(j)
        first_left(j)

    for k in range(2, n_head):
        finish((me + k) % n_head) if k < n_head - 1 else finish(me)
    for k in range(1, n_head):
        square_copy(k, me).start()

    for step in range(1, n_head - 1):
        block_r, block_l = (me + 2 * n_head - 1 - step) % n_head, (me + 1 + step) % n_head

        @pl.loop(0, parts)
        def _(j):
            own = product(block_r, j * cut)
            right_copy(step - 1, j).wait_recv()
            send_r[step, j] = (own + got_r[step - 1, j].astype(F32)).astype(BF16)
            right_copy(step, j).start()
            own = product(block_l, out_width // 2 + j * cut)
            left_copy(step - 1, j).wait_recv()
            send_l[step, j] = (own + got_l[step - 1, j].astype(F32)).astype(BF16)
            left_copy(step, j).start()

    total = sq_ref[me]
    for k in range(1, n_head):
        owner = (me + n_head - k) % n_head
        square_copy(k, owner).wait_recv()
        total = total + got_sq[owner]
    inverse_rms = lax.rsqrt(total / (width * n_head) + NORM_EPS).T[:, :1]

    @pl.loop(0, parts)
    def _(j):
        last = n_head - 2
        own = product(me, j * cut)
        right_copy(last, j).wait_recv()
        own = (own + got_r[last, j].astype(F32)) * inverse_rms
        out_ref[:, pl.ds(pl.multiple_of(j * cut, cut), cut)] = own.astype(BF16)
        column = out_width // 2 + j * cut
        own = product(me, column)
        left_copy(last, j).wait_recv()
        own = (own + got_l[last, j].astype(F32)) * inverse_rms
        out_ref[:, pl.ds(pl.multiple_of(column, cut), cut)] = own.astype(BF16)

    for k in range(1, n_head):
        for what in range(2):
            bc_copy(k, what, me).wait_send()
        square_copy(k, me).wait_send()

    @pl.loop(1, line)
    def _(k):
        decay_copy(k, place).wait_send()
        state_copy(k, place).wait_send()
        back_copy(k, place).wait_send()

    line_copy.wait_send()
    for step in range(n_head - 1):

        @pl.loop(0, parts)
        def _(j):
            right_copy(step, j).wait_send()
            left_copy(step, j).wait_send()


def on_device(sizes, x_in, z_gate, b_in, c_in, dt_raw, decay_rate, skip_gain, norm_gain, w_out, doc_lengths):
    n_head, n_seq, line = sizes
    rows, width = x_in.shape
    heads = dt_raw.shape[1]
    out_width = w_out.shape[1]
    state_size = b_in.shape[1] * n_head
    spans = rows // SPAN
    part, half = state_size * 2 // line, width // 2
    parts = 5
    cut = out_width // 2 // parts
    ring = (n_head - 1, parts, rows // n_head, cut)
    vmem, anywhere = pl.BlockSpec(memory_space=pltpu.VMEM), pl.BlockSpec(memory_space=pl.ANY)
    dma = pltpu.SemaphoreType.DMA
    result = pl.pallas_call(
        functools.partial(layer_kernel, sizes),
        out_shape=pltpu.VMEM((rows // n_head, out_width), BF16),
        in_specs=[anywhere] * 10,
        out_specs=vmem,
        scratch_shapes=[
            pltpu.VMEM((state_size // n_head, rows), BF16),
            pltpu.VMEM((state_size // n_head, rows), BF16),
            pltpu.VMEM((heads, rows), F32),
            pltpu.VMEM((1, heads), F32),
            pltpu.VMEM((1, heads), F32),
            pltpu.VMEM((1, width), F32),
            pltpu.VMEM((1, doc_lengths.shape[0]), jnp.int32),
            pltpu.VMEM((rows, width), BF16),
            pltpu.VMEM((rows, width), BF16),
            pltpu.VMEM(w_out.shape, BF16),
            pltpu.VMEM((state_size, rows), BF16),
            pltpu.VMEM((state_size, rows), BF16),
            pltpu.VMEM((rows, width), BF16),
            pltpu.VMEM((heads, rows), F32),
            pltpu.VMEM((spans * 16, width), F32),
            pltpu.VMEM((spans, state_size, width), F32),
            pltpu.VMEM((rows, width), F32),
            pltpu.VMEM((rows, width), F32),
            pltpu.VMEM((state_size, width), BF16),
            pltpu.VMEM((8, 128), F32),
            pltpu.VMEM((line, part, half), BF16),
            pltpu.VMEM((line, 8, 128), F32),
            pltpu.VMEM((part, half), F32),
            pltpu.VMEM((part, half), F32),
            pltpu.VMEM((line, part, half), BF16),
            pltpu.VMEM((state_size, width), BF16),
            pltpu.VMEM((rows, width), BF16),
            pltpu.VMEM((n_head, 8, SPAN), F32),
            pltpu.VMEM((n_head, 8, SPAN), F32),
            pltpu.VMEM(ring, BF16),
            pltpu.VMEM(ring, BF16),
            pltpu.VMEM(ring, BF16),
            pltpu.VMEM(ring, BF16),
            pltpu.VMEM((line * 8, half), F32),
            dma((10,)),
            dma((2, n_head)),
            dma((2, n_head)),
            dma((line,)),
            dma((line,)),
            dma((line,)),
            dma((line,)),
            dma,
            dma,
            dma((line,)),
            dma((line,)),
            dma((n_head,)),
            dma((n_head,)),
            dma((n_head - 1, parts)),
            dma((n_head - 1, parts)),
            dma((n_head - 1, parts)),
            dma((n_head - 1, parts)),
        ],
        compiler_params=pltpu.CompilerParams(
            collective_id=0, has_side_effects=True, vmem_limit_bytes=60 * 1024 * 1024
        ),
        name="ssd_layer",
    )(
        b_in.T,
        c_in.T,
        dt_raw.T,
        decay_rate[None, :],
        skip_gain[None, :],
        norm_gain[None, :],
        doc_lengths[None, :],
        x_in,
        z_gate,
        w_out,
    )
    return result


def solution(mesh):
    sizes = (mesh.shape["head"], mesh.shape["seq"], 16)
    rows = P("seq", "head")
    return jax.shard_map(
        functools.partial(on_device, sizes),
        mesh=mesh,
        in_specs=(rows, rows, rows, rows, rows, P("head"), P("head"), P("head"), P("head", None), P()),
        out_specs=P(("seq", "head"), None),
        check_vma=False,
    )
```

```python
import functools

import jax
import jax.numpy as jnp
from jax import lax
from jax.experimental import pallas as pl
from jax.experimental.pallas import tpu as pltpu
from jax.sharding import PartitionSpec as P

SPAN = 256
NORM_EPS = 1e-05
MESH = pl.DeviceIdType.MESH
F32 = jnp.float32
BF16 = jnp.bfloat16


def pieces(v, terms):
    out = []
    for _ in range(terms):
        part = v.astype(BF16)
        out.append(part)
        v = v - part.astype(F32)
    return out


def expand(v, spread, terms=2):
    total = None
    for part in pieces(v, terms):
        term = lax.dot_general(part, spread, (((0,), (0,)), ((), ())), preferred_element_type=F32)
        total = term if total is None else total + term
    return total


def iota(shape, dim):
    return lax.broadcasted_iota(jnp.int32, shape, dim)


def layer_kernel(
    sizes,
    b_hbm, c_hbm, dt_hbm, rate_hbm, skip_hbm, gain_hbm, docs_hbm, x_hbm, z_hbm, w_hbm,
    out_ref,
    b_ref, c_ref, dt_ref, rate_ref, skip_ref, gain_ref, docs_ref, x_ref, z_ref, w_ref, bt_ref, ct_ref, xf_ref, e_ref, rows_ref, before_ref, ur_ref, as_ref,
    state_ref, decay_ref, got_state, got_decay, line_ref, got_line, back_ref, inc_ref, norm_ref,
    sq_ref, got_sq, send_r, got_r, send_l, got_l, decays_ref, cn_ref, folded_ref, own_state_ref,
    in_sem, bc_send, bc_recv, st_send, st_recv, dc_send, dc_recv, ln_send, ln_recv, bk_send, bk_recv,
    sq_send, sq_recv, r_send, r_recv, l_send, l_recv,
):
    n_head, n_seq, line = sizes
    rows, width = x_ref.shape
    heads = dt_ref.shape[0]
    head_size = width // heads
    state_size = bt_ref.shape[0]
    piece = b_ref.shape[0]
    spans = rows // SPAN
    me, seq = lax.axis_index("head"), lax.axis_index("seq")
    at_line, place = seq // line, seq % line
    first = seq - place
    half = width // 2
    part = state_size * 2 // line

    def load(i, src, dst):
        return pltpu.make_async_copy(src, dst, in_sem.at[i])

    barrier = pltpu.get_barrier_semaphore()
    for k in range(1, n_head):
        pl.semaphore_signal(barrier, inc=1, device_id={"head": (me + k) % n_head}, device_id_type=MESH)

    @pl.loop(1, line)
    def _(k):
        pl.semaphore_signal(
            barrier, inc=1, device_id={"seq": first + (place + k) % line}, device_id_type=MESH
        )

    for step in (line, n_seq - line):
        pl.semaphore_signal(barrier, inc=1, device_id={"seq": (seq + step) % n_seq}, device_id_type=MESH)
    sources = (b_hbm, dt_hbm, rate_hbm, docs_hbm, x_hbm, c_hbm, skip_hbm, gain_hbm, z_hbm, w_hbm)
    targets = (b_ref, dt_ref, rate_ref, docs_ref, x_ref, c_ref, skip_ref, gain_ref, z_ref, w_ref)
    loads = [load(i, *pair) for i, pair in enumerate(zip(sources, targets))]
    for one in loads:
        one.start()
    for one in loads[:4]:
        one.wait()
    loads[5].wait()
    pl.semaphore_wait(barrier, n_head - 1 + line - 1 + 2)

    def bc_copy(k, what, owner):
        dst = (bt_ref, ct_ref)[what].at[pl.ds(pl.multiple_of(owner * piece, piece), piece), :]
        return pltpu.make_async_remote_copy(
            src_ref=(b_ref, c_ref)[what],
            dst_ref=dst,
            send_sem=bc_send.at[what, k],
            recv_sem=bc_recv.at[what, owner],
            device_id={"head": (me + k) % n_head},
            device_id_type=MESH,
        )

    for what in range(2):
        for k in (2, 1, n_head - 1):
            bc_copy(k, what, me).start()
        mine = pl.ds(pl.multiple_of(me * piece, piece), piece)
        (bt_ref, ct_ref)[what][mine, :] = (b_ref, c_ref)[what][...]

    n_docs = docs_ref.shape[1]
    lengths = jnp.broadcast_to(docs_ref[...].astype(F32), (n_docs, n_docs))
    up, across = iota((n_docs, n_docs), 0), iota((n_docs, n_docs), 1)
    ends_col = jnp.sum(jnp.where(across <= up, lengths, 0.0), axis=1, keepdims=True)
    lengths_col = jnp.sum(jnp.where(across == up, lengths, 0.0), axis=1, keepdims=True)
    ends_row = jnp.sum(
        jnp.where(up <= across, jnp.broadcast_to(lengths_col, (n_docs, n_docs)), 0.0), axis=0, keepdims=True
    )

    def id_of(position):
        return jnp.sum(jnp.where(position >= ends_row, 1.0, 0.0), axis=1, keepdims=True)

    def ids_of(s):
        start = seq * rows + s * SPAN
        col = id_of((start + iota((SPAN, 1), 0)).astype(F32))
        row = jnp.sum(
            jnp.where((start + iota((1, SPAN), 1)).astype(F32) >= ends_col, 1.0, 0.0), axis=0, keepdims=True
        )
        ahead = start - 1 + iota((1, 1), 0)
        previous = id_of(ahead.astype(F32)) - jnp.where(ahead < 0, 1.0, 0.0)
        last = id_of((start + SPAN - 1 + iota((1, 1), 0)).astype(F32))
        return col, row, previous, last

    spread = (iota((heads, width), 1) // head_size == iota((heads, width), 0)).astype(BF16)
    own_lane = iota((heads, heads), 0) == iota((heads, heads), 1)
    rate = jnp.sum(jnp.where(own_lane, rate_ref[...], 0.0), axis=1, keepdims=True)
    upto = (iota((SPAN, SPAN), 0) <= iota((SPAN, SPAN), 1)).astype(BF16)

    loads[4].wait()

    def scale_span(s, device_decay):
        at = pl.ds(pl.multiple_of(s * SPAN, SPAN), SPAN)
        raw = dt_ref[:, at]
        step = jnp.maximum(raw, 0.0) + jnp.log(1.0 + jnp.exp(-jnp.abs(raw)))
        cum = None
        for term in pieces(-step * rate, 3):
            sums = jnp.dot(term, upto, preferred_element_type=F32)
            cum = sums if cum is None else cum + sums
        middle = 0.5 * cum[:, SPAN - 1 :]
        e_ref[:, at] = jnp.exp(cum - middle)
        forward = step * jnp.exp(middle - cum)
        xf_ref[at, :] = (x_ref[at, :].astype(F32) * expand(forward, spread)).astype(BF16)
        _, _, previous, last = ids_of(s)
        total = jnp.exp(2.0 * middle) * jnp.where(last == previous, 1.0, 0.0)
        both = jnp.where(iota((heads, 16), 1) < 8, jnp.exp(middle), total)
        rows_ref[pl.ds(pl.multiple_of(s * 16, 16), 16), :] = expand(both, spread, 3)
        return device_decay * total

    device_decay = lax.fori_loop(0, spans, scale_span, jnp.ones((heads, 1), F32))
    decay_ref[...] = jnp.zeros_like(decay_ref)
    decay_ref[:, :heads] = jnp.broadcast_to(device_decay, (heads, 128)).T[:8, :]

    def farthest_first(i):
        return line // 2 + jnp.where(i % 2 == 0, i // 2, -(i // 2))

    def line_peer(k):
        return {"seq": first + (place + k) % line}

    def from_peer(k):
        return (place + line - k) % line

    def decay_copy(k, owner):
        return pltpu.make_async_remote_copy(
            src_ref=decay_ref,
            dst_ref=got_decay.at[owner],
            send_sem=dc_send.at[k],
            recv_sem=dc_recv.at[owner],
            device_id=line_peer(k),
            device_id_type=MESH,
        )

    @pl.loop(1, line)
    def _(k):
        decay_copy(k, place).start()

    got_decay[place] = decay_ref[...]

    for k in range(1, n_head):
        bc_copy(k, 0, (me + n_head - k) % n_head).wait_recv()

    def state_span(s, running):
        at = pl.ds(pl.multiple_of(s * SPAN, SPAN), SPAN)
        before_ref[s] = running
        _, row, _, last = ids_of(s)
        kept = jnp.where(row == last, bt_ref[:, at].astype(F32), 0.0).astype(BF16)
        sums = jnp.dot(kept, xf_ref[at, :], preferred_element_type=F32)
        base = pl.multiple_of(s * 16, 16)
        return rows_ref[pl.ds(base + 8, 1), :] * running + sums * rows_ref[pl.ds(base, 1), :]

    final = lax.fori_loop(0, spans, state_span, jnp.zeros((state_size, width), F32))
    state_ref[...] = final.astype(BF16)

    def own_part(t):
        return (
            pl.ds(pl.multiple_of((t // 2) * part, part), part),
            pl.ds(pl.multiple_of((t % 2) * half, half), half),
        )

    def state_copy(k, owner):
        to = (place + k) % line
        return pltpu.make_async_remote_copy(
            src_ref=state_ref.at[own_part(to)],
            dst_ref=got_state.at[owner],
            send_sem=st_send.at[k],
            recv_sem=st_recv.at[owner],
            device_id=line_peer(k),
            device_id_type=MESH,
        )

    @pl.loop(1, line)
    def _(i):
        state_copy(farthest_first(i), place).start()

    got_state[place] = state_ref[own_part(place)]

    @pl.loop(1, line)
    def _(k):
        decay_copy(k, from_peer(k)).wait_recv()

    lanes = iota((128, half), 1) + (place % 2) * half
    spread_here = (lanes // head_size == iota((128, half), 0)).astype(BF16)
    decays_ref[...] = expand(got_decay[...].reshape(line * 8, 128).T, spread_here, 3)
    @pl.loop(1, line)
    def _(k):
        state_copy(k, from_peer(k)).wait_recv()

    inside, inc = [], jnp.zeros((part, half), F32)
    for d in range(line):
        inside.append(inc)
        inc = decays_ref[8 * d : 8 * d + 1, :] * inc + got_state[d].astype(F32)
    line_ref[...] = inc
    line_copy = pltpu.make_async_remote_copy(
        src_ref=line_ref,
        dst_ref=got_line,
        send_sem=ln_send,
        recv_sem=ln_recv,
        device_id={"seq": (seq + line) % n_seq},
        device_id_type=MESH,
    )
    pl.when(at_line < n_seq // line - 1)(line_copy.start)

    @pl.when(at_line > 0)
    def _():
        line_copy.wait_recv()

    @pl.when(at_line == 0)
    def _():
        got_line[...] = jnp.zeros_like(got_line)

    factor = jnp.ones((1, half), F32)
    earlier = got_line[...]
    for d in range(line):
        back_ref[d] = (inside[d] + factor * earlier).astype(BF16)
        factor = factor * decays_ref[8 * d : 8 * d + 1, :]

    def back_copy(k, owner):
        return pltpu.make_async_remote_copy(
            src_ref=back_ref.at[(place + k) % line],
            dst_ref=inc_ref.at[own_part(owner)],
            send_sem=bk_send.at[k],
            recv_sem=bk_recv.at[owner],
            device_id=line_peer(k),
            device_id_type=MESH,
        )

    @pl.loop(1, line)
    def _(i):
        back_copy(farthest_first(i), place).start()

    inc_ref[own_part(place)] = back_ref[place]

    for k in range(1, n_head):
        bc_copy(k, 1, (me + n_head - k) % n_head).wait_recv()
    for one in loads[6:9]:
        one.wait()
    skip = jnp.sum(jnp.where(own_lane, skip_ref[...], 0.0), axis=1, keepdims=True)
    skip_row = expand(jnp.broadcast_to(skip, (heads, 8)), spread, 3)[:1, :]

    @pl.loop(0, spans)
    def _(s):
        at = pl.ds(pl.multiple_of(s * SPAN, SPAN), SPAN)
        col, row, previous, _ = ids_of(s)
        c_here = ct_ref[:, at].T
        cn_ref[at, :] = c_here
        scores = jnp.dot(c_here, bt_ref[:, at], preferred_element_type=F32)
        seen = (col == row) & (iota((SPAN, SPAN), 0) >= iota((SPAN, SPAN), 1))
        scores = jnp.where(seen, scores, 0.0).astype(BF16)
        local = jnp.dot(scores, xf_ref[at, :], preferred_element_type=F32)
        inter = jnp.dot(c_here, before_ref[s].astype(BF16), preferred_element_type=F32)
        base = pl.multiple_of(s * 16, 16)
        out_of_middle = expand(e_ref[:, at], spread)
        from_start = rows_ref[pl.ds(base, 1), :] * jnp.where(col == previous, 1.0, 0.0)
        gate = z_ref[at, :].astype(F32)
        gate = gate / (1.0 + jnp.exp(-gate))
        y = out_of_middle * (local + from_start * inter) + skip_row * x_ref[at, :].astype(F32)
        ur_ref[at, :] = y * gate
        as_ref[at, :] = out_of_middle * from_start * gate

    loads[9].wait()

    @pl.loop(1, line)
    def _(k):
        back_copy(k, from_peer(k)).wait_recv()

    def finish(block):
        at = pl.ds(pl.multiple_of(block * SPAN, SPAN), SPAN)
        before = jnp.ones((1, width), F32)
        for s in range(spans - 1):
            decay = rows_ref[16 * s + 8 : 16 * s + 9, :]
            before = jnp.where(s + iota((1, width), 0) < block, before * decay, before)
        carried = (inc_ref[...].astype(F32) * before).astype(BF16)
        inter = jnp.dot(cn_ref[at, :], carried, preferred_element_type=F32)
        gated = ur_ref[at, :] + as_ref[at, :] * inter
        norm_ref[at, :] = (gated * gain_ref[...]).astype(BF16)
        squares = gated * gated
        folded = squares[:, :128]
        for j in range(1, width // 128):
            folded = folded + squares[:, 128 * j : 128 * (j + 1)]
        folded_ref[at, :] = folded

    def square_rows(block):
        folded = folded_ref[pl.ds(pl.multiple_of(block * SPAN, SPAN), SPAN), :]
        sq_ref[block] = jnp.broadcast_to(jnp.sum(folded.T, axis=0, keepdims=True), (8, SPAN))

    def square_copy(k, owner):
        return pltpu.make_async_remote_copy(
            src_ref=sq_ref.at[(me + k) % n_head],
            dst_ref=got_sq.at[owner],
            send_sem=sq_send.at[k],
            recv_sem=sq_recv.at[owner],
            device_id={"head": (me + k) % n_head},
            device_id_type=MESH,
        )

    out_width = out_ref.shape[1]
    parts, cut = got_r.shape[1], got_r.shape[3]

    def product(block, column):
        return jnp.dot(
            norm_ref[pl.ds(pl.multiple_of(block * SPAN, SPAN), SPAN), :],
            w_ref[:, pl.ds(pl.multiple_of(column, cut), cut)],
            preferred_element_type=F32,
        )

    def right_copy(step, j):
        return pltpu.make_async_remote_copy(
            src_ref=send_r.at[step, j],
            dst_ref=got_r.at[step, j],
            send_sem=r_send.at[step, j],
            recv_sem=r_recv.at[step, j],
            device_id={"head": (me + 1) % n_head},
            device_id_type=MESH,
        )

    def left_copy(step, j):
        return pltpu.make_async_remote_copy(
            src_ref=send_l.at[step, j],
            dst_ref=got_l.at[step, j],
            send_sem=l_send.at[step, j],
            recv_sem=l_recv.at[step, j],
            device_id={"head": (me + n_head - 1) % n_head},
            device_id_type=MESH,
        )

    ahead, behind = (me + n_head - 1) % n_head, (me + 1) % n_head
    def first_right(j):
        send_r[0, j] = product(ahead, j * cut).astype(BF16)
        right_copy(0, j).start()

    def first_left(j):
        send_l[0, j] = product(behind, out_width // 2 + j * cut).astype(BF16)
        left_copy(0, j).start()

    finish(ahead)
    first_right(0)
    finish(behind)
    first_left(0)

    @pl.loop(1, parts)
    def _(j):
        first_right(j)
        first_left(j)

    for k in range(2, n_head):
        finish((me + k) % n_head) if k < n_head - 1 else finish(me)
    for k in range(n_head):
        square_rows((me + k) % n_head)
    for k in range(1, n_head):
        square_copy(k, me).start()

    for step in range(1, n_head - 1):
        block_r, block_l = (me + 2 * n_head - 1 - step) % n_head, (me + 1 + step) % n_head

        @pl.loop(0, parts)
        def _(j):
            own = product(block_r, j * cut)
            right_copy(step - 1, j).wait_recv()
            send_r[step, j] = (own + got_r[step - 1, j].astype(F32)).astype(BF16)
            right_copy(step, j).start()
            own = product(block_l, out_width // 2 + j * cut)
            left_copy(step - 1, j).wait_recv()
            send_l[step, j] = (own + got_l[step - 1, j].astype(F32)).astype(BF16)
            left_copy(step, j).start()

    total = sq_ref[me]
    for k in range(1, n_head):
        owner = (me + n_head - k) % n_head
        square_copy(k, owner).wait_recv()
        total = total + got_sq[owner]
    inverse_rms = lax.rsqrt(total / (width * n_head) + NORM_EPS).T[:, :1]

    @pl.loop(0, parts)
    def _(j):
        last = n_head - 2
        own = product(me, j * cut)
        right_copy(last, j).wait_recv()
        own = (own + got_r[last, j].astype(F32)) * inverse_rms
        out_ref[:, pl.ds(pl.multiple_of(j * cut, cut), cut)] = own.astype(BF16)
        column = out_width // 2 + j * cut
        own = product(me, column)
        left_copy(last, j).wait_recv()
        own = (own + got_l[last, j].astype(F32)) * inverse_rms
        out_ref[:, pl.ds(pl.multiple_of(column, cut), cut)] = own.astype(BF16)

    for k in range(1, n_head):
        for what in range(2):
            bc_copy(k, what, me).wait_send()
        square_copy(k, me).wait_send()

    @pl.loop(1, line)
    def _(k):
        decay_copy(k, place).wait_send()
        state_copy(k, place).wait_send()
        back_copy(k, place).wait_send()

    pl.when(at_line < n_seq // line - 1)(line_copy.wait_send)
    for step in range(n_head - 1):

        @pl.loop(0, parts)
        def _(j):
            right_copy(step, j).wait_send()
            left_copy(step, j).wait_send()


def on_device(sizes, x_in, z_gate, b_in, c_in, dt_raw, decay_rate, skip_gain, norm_gain, w_out, doc_lengths):
    n_head, n_seq, line = sizes
    rows, width = x_in.shape
    heads = dt_raw.shape[1]
    out_width = w_out.shape[1]
    state_size = b_in.shape[1] * n_head
    spans = rows // SPAN
    part, half = state_size * 2 // line, width // 2
    parts = 5
    cut = out_width // 2 // parts
    ring = (n_head - 1, parts, rows // n_head, cut)
    vmem, anywhere = pl.BlockSpec(memory_space=pltpu.VMEM), pl.BlockSpec(memory_space=pl.ANY)
    dma = pltpu.SemaphoreType.DMA
    result = pl.pallas_call(
        functools.partial(layer_kernel, sizes),
        out_shape=pltpu.VMEM((rows // n_head, out_width), BF16),
        in_specs=[anywhere] * 10,
        out_specs=vmem,
        scratch_shapes=[
            pltpu.VMEM((state_size // n_head, rows), BF16),
            pltpu.VMEM((state_size // n_head, rows), BF16),
            pltpu.VMEM((heads, rows), F32),
            pltpu.VMEM((1, heads), F32),
            pltpu.VMEM((1, heads), F32),
            pltpu.VMEM((1, width), F32),
            pltpu.VMEM((1, doc_lengths.shape[0]), jnp.int32),
            pltpu.VMEM((rows, width), BF16),
            pltpu.VMEM((rows, width), BF16),
            pltpu.VMEM(w_out.shape, BF16),
            pltpu.VMEM((state_size, rows), BF16),
            pltpu.VMEM((state_size, rows), BF16),
            pltpu.VMEM((rows, width), BF16),
            pltpu.VMEM((heads, rows), F32),
            pltpu.VMEM((spans * 16, width), F32),
            pltpu.VMEM((spans, state_size, width), F32),
            pltpu.VMEM((rows, width), F32),
            pltpu.VMEM((rows, width), F32),
            pltpu.VMEM((state_size, width), BF16),
            pltpu.VMEM((8, 128), F32),
            pltpu.VMEM((line, part, half), BF16),
            pltpu.VMEM((line, 8, 128), F32),
            pltpu.VMEM((part, half), F32),
            pltpu.VMEM((part, half), F32),
            pltpu.VMEM((line, part, half), BF16),
            pltpu.VMEM((state_size, width), BF16),
            pltpu.VMEM((rows, width), BF16),
            pltpu.VMEM((n_head, 8, SPAN), F32),
            pltpu.VMEM((n_head, 8, SPAN), F32),
            pltpu.VMEM(ring, BF16),
            pltpu.VMEM(ring, BF16),
            pltpu.VMEM(ring, BF16),
            pltpu.VMEM(ring, BF16),
            pltpu.VMEM((line * 8, half), F32),
            pltpu.VMEM((rows, state_size), BF16),
            pltpu.VMEM((rows, 128), F32),
            pltpu.VMEM((state_size // n_head, width), BF16),
            dma((10,)),
            dma((2, n_head)),
            dma((2, n_head)),
            dma((line,)),
            dma((line,)),
            dma((line,)),
            dma((line,)),
            dma,
            dma,
            dma((line,)),
            dma((line,)),
            dma((n_head,)),
            dma((n_head,)),
            dma((n_head - 1, parts)),
            dma((n_head - 1, parts)),
            dma((n_head - 1, parts)),
            dma((n_head - 1, parts)),
        ],
        compiler_params=pltpu.CompilerParams(
            collective_id=0, has_side_effects=True, vmem_limit_bytes=60 * 1024 * 1024
        ),
        name="ssd_layer",
    )(
        b_in.T,
        c_in.T,
        dt_raw.T,
        decay_rate[None, :],
        skip_gain[None, :],
        norm_gain[None, :],
        doc_lengths[None, :],
        x_in,
        z_gate,
        w_out,
    )
    return result


def solution(mesh):
    sizes = (mesh.shape["head"], mesh.shape["seq"], 16)
    rows = P("seq", "head")
    return jax.shard_map(
        functools.partial(on_device, sizes),
        mesh=mesh,
        in_specs=(rows, rows, rows, rows, rows, P("head"), P("head"), P("head"), P("head", None), P()),
        out_specs=P(("seq", "head"), None),
        check_vma=False,
    )
```

```python
import functools

import jax
import jax.numpy as jnp
from jax import lax
from jax.experimental import pallas as pl
from jax.experimental.pallas import tpu as pltpu
from jax.sharding import PartitionSpec as P

SPAN = 256
NORM_EPS = 1e-05
MESH = pl.DeviceIdType.MESH
F32 = jnp.float32
BF16 = jnp.bfloat16


def pieces(v, terms):
    out = []
    for _ in range(terms):
        part = v.astype(BF16)
        out.append(part)
        v = v - part.astype(F32)
    return out


def expand(v, spread, terms=2):
    total = None
    for part in pieces(v, terms):
        term = lax.dot_general(part, spread, (((0,), (0,)), ((), ())), preferred_element_type=F32)
        total = term if total is None else total + term
    return total


def iota(shape, dim):
    return lax.broadcasted_iota(jnp.int32, shape, dim)


def layer_kernel(
    sizes,
    b_hbm, c_hbm, dt_hbm, rate_hbm, skip_hbm, gain_hbm, docs_hbm, x_hbm, z_hbm, w_hbm,
    out_ref,
    b_ref, c_ref, dt_ref, rate_ref, skip_ref, gain_ref, docs_ref, x_ref, z_ref, w_ref, bt_ref, ct_ref, xf_ref, e_ref, rows_ref, before_ref, ur_ref, as_ref,
    state_ref, decay_ref, got_state, got_decay, line_ref, got_line, back_ref, inc_ref, norm_ref,
    sq_ref, got_sq, send_r, got_r, send_l, got_l, decays_ref, cn_ref, folded_ref, kept_ref,
    in_sem, bc_send, bc_recv, st_send, st_recv, dc_send, dc_recv, ln_send, ln_recv, bk_send, bk_recv,
    sq_send, sq_recv, r_send, r_recv, l_send, l_recv,
):
    n_head, n_seq, line = sizes
    rows, width = x_ref.shape
    heads = dt_ref.shape[0]
    head_size = width // heads
    state_size = bt_ref.shape[0]
    piece = b_ref.shape[0]
    spans = rows // SPAN
    me, seq = lax.axis_index("head"), lax.axis_index("seq")
    at_line, place = seq // line, seq % line
    first = seq - place
    half = width // 2
    part = state_size * 2 // line

    def load(i, src, dst):
        return pltpu.make_async_copy(src, dst, in_sem.at[i])

    barrier = pltpu.get_barrier_semaphore()
    for k in range(1, n_head):
        pl.semaphore_signal(barrier, inc=1, device_id={"head": (me + k) % n_head}, device_id_type=MESH)

    @pl.loop(1, line)
    def _(k):
        pl.semaphore_signal(
            barrier, inc=1, device_id={"seq": first + (place + k) % line}, device_id_type=MESH
        )

    for step in (line, n_seq - line):
        pl.semaphore_signal(barrier, inc=1, device_id={"seq": (seq + step) % n_seq}, device_id_type=MESH)
    sources = (b_hbm, dt_hbm, rate_hbm, docs_hbm, x_hbm, c_hbm, skip_hbm, gain_hbm, z_hbm, w_hbm)
    targets = (b_ref, dt_ref, rate_ref, docs_ref, x_ref, c_ref, skip_ref, gain_ref, z_ref, w_ref)
    loads = [load(i, *pair) for i, pair in enumerate(zip(sources, targets))]
    for one in loads:
        one.start()
    for one in loads[:4]:
        one.wait()
    loads[5].wait()
    pl.semaphore_wait(barrier, n_head - 1 + line - 1 + 2)

    def bc_copy(k, what, owner):
        dst = (bt_ref, ct_ref)[what].at[pl.ds(pl.multiple_of(owner * piece, piece), piece), :]
        return pltpu.make_async_remote_copy(
            src_ref=(b_ref, c_ref)[what],
            dst_ref=dst,
            send_sem=bc_send.at[what, k],
            recv_sem=bc_recv.at[what, owner],
            device_id={"head": (me + k) % n_head},
            device_id_type=MESH,
        )

    for what in range(2):
        for k in (2, 1, n_head - 1):
            bc_copy(k, what, me).start()
        mine = pl.ds(pl.multiple_of(me * piece, piece), piece)
        (bt_ref, ct_ref)[what][mine, :] = (b_ref, c_ref)[what][...]

    n_docs = docs_ref.shape[1]
    lengths = jnp.broadcast_to(docs_ref[...].astype(F32), (n_docs, n_docs))
    up, across = iota((n_docs, n_docs), 0), iota((n_docs, n_docs), 1)
    ends_col = jnp.sum(jnp.where(across <= up, lengths, 0.0), axis=1, keepdims=True)
    lengths_col = jnp.sum(jnp.where(across == up, lengths, 0.0), axis=1, keepdims=True)
    ends_row = jnp.sum(
        jnp.where(up <= across, jnp.broadcast_to(lengths_col, (n_docs, n_docs)), 0.0), axis=0, keepdims=True
    )

    def id_of(position):
        return jnp.sum(jnp.where(position >= ends_row, 1.0, 0.0), axis=1, keepdims=True)

    def ids_of(s):
        start = seq * rows + s * SPAN
        col = id_of((start + iota((SPAN, 1), 0)).astype(F32))
        row = jnp.sum(
            jnp.where((start + iota((1, SPAN), 1)).astype(F32) >= ends_col, 1.0, 0.0), axis=0, keepdims=True
        )
        ahead = start - 1 + iota((1, 1), 0)
        previous = id_of(ahead.astype(F32)) - jnp.where(ahead < 0, 1.0, 0.0)
        last = id_of((start + SPAN - 1 + iota((1, 1), 0)).astype(F32))
        return col, row, previous, last

    spread = (iota((heads, width), 1) // head_size == iota((heads, width), 0)).astype(BF16)
    own_lane = iota((heads, heads), 0) == iota((heads, heads), 1)
    rate = jnp.sum(jnp.where(own_lane, rate_ref[...], 0.0), axis=1, keepdims=True)
    upto = (iota((SPAN, SPAN), 0) <= iota((SPAN, SPAN), 1)).astype(BF16)

    loads[4].wait()

    def scale_span(s, device_decay):
        at = pl.ds(pl.multiple_of(s * SPAN, SPAN), SPAN)
        raw = dt_ref[:, at]
        step = jnp.maximum(raw, 0.0) + jnp.log(1.0 + jnp.exp(-jnp.abs(raw)))
        cum = None
        for term in pieces(-step * rate, 3):
            sums = jnp.dot(term, upto, preferred_element_type=F32)
            cum = sums if cum is None else cum + sums
        middle = 0.5 * cum[:, SPAN - 1 :]
        e_ref[:, at] = jnp.exp(cum - middle)
        forward = step * jnp.exp(middle - cum)
        xf_ref[at, :] = (x_ref[at, :].astype(F32) * expand(forward, spread)).astype(BF16)
        _, _, previous, last = ids_of(s)
        total = jnp.exp(2.0 * middle) * jnp.where(last == previous, 1.0, 0.0)
        both = jnp.where(iota((heads, 16), 1) < 8, jnp.exp(middle), total)
        rows_ref[pl.ds(pl.multiple_of(s * 16, 16), 16), :] = expand(both, spread, 3)
        return device_decay * total

    device_decay = lax.fori_loop(0, spans, scale_span, jnp.ones((heads, 1), F32))
    decay_ref[...] = jnp.zeros_like(decay_ref)
    decay_ref[:, :heads] = jnp.broadcast_to(device_decay, (heads, 128)).T[:8, :]

    def farthest_first(i):
        return line // 2 + jnp.where(i % 2 == 0, i // 2, -(i // 2))

    def line_peer(k):
        return {"seq": first + (place + k) % line}

    def from_peer(k):
        return (place + line - k) % line

    def decay_copy(k, owner):
        return pltpu.make_async_remote_copy(
            src_ref=decay_ref,
            dst_ref=got_decay.at[owner],
            send_sem=dc_send.at[k],
            recv_sem=dc_recv.at[owner],
            device_id=line_peer(k),
            device_id_type=MESH,
        )

    @pl.loop(1, line)
    def _(k):
        decay_copy(k, place).start()

    got_decay[place] = decay_ref[...]

    for k in range(1, n_head):
        bc_copy(k, 0, (me + n_head - k) % n_head).wait_recv()

    for s in range(spans):
        _, row, _, last = ids_of(s)
        at = slice(s * SPAN, (s + 1) * SPAN)
        kept_ref[:, at] = jnp.where(row == last, bt_ref[:, at].astype(F32), 0.0).astype(BF16)

    @pl.loop(0, width // SPAN)
    def _(n):
        lanes_here = pl.ds(pl.multiple_of(n * SPAN, SPAN), SPAN)
        running = jnp.zeros((state_size, SPAN), F32)
        for s in range(spans):
            at = slice(s * SPAN, (s + 1) * SPAN)
            before_ref[s, :, lanes_here] = running
            sums = jnp.dot(kept_ref[:, at], xf_ref[at, lanes_here], preferred_element_type=F32)
            to_last = rows_ref[16 * s : 16 * s + 1, lanes_here]
            running = rows_ref[16 * s + 8 : 16 * s + 9, lanes_here] * running + sums * to_last
        state_ref[:, lanes_here] = running.astype(BF16)

    def own_part(t):
        return (
            pl.ds(pl.multiple_of((t // 2) * part, part), part),
            pl.ds(pl.multiple_of((t % 2) * half, half), half),
        )

    def state_copy(k, owner):
        to = (place + k) % line
        return pltpu.make_async_remote_copy(
            src_ref=state_ref.at[own_part(to)],
            dst_ref=got_state.at[owner],
            send_sem=st_send.at[k],
            recv_sem=st_recv.at[owner],
            device_id=line_peer(k),
            device_id_type=MESH,
        )

    @pl.loop(1, line)
    def _(i):
        state_copy(farthest_first(i), place).start()

    got_state[place] = state_ref[own_part(place)]

    @pl.loop(1, line)
    def _(k):
        decay_copy(k, from_peer(k)).wait_recv()

    lanes = iota((128, half), 1) + (place % 2) * half
    spread_here = (lanes // head_size == iota((128, half), 0)).astype(BF16)
    decays_ref[...] = expand(got_decay[...].reshape(line * 8, 128).T, spread_here, 3)
    @pl.loop(1, line)
    def _(k):
        state_copy(k, from_peer(k)).wait_recv()

    inside, inc = [], jnp.zeros((part, half), F32)
    for d in range(line):
        inside.append(inc)
        inc = decays_ref[8 * d : 8 * d + 1, :] * inc + got_state[d].astype(F32)
    line_ref[...] = inc
    line_copy = pltpu.make_async_remote_copy(
        src_ref=line_ref,
        dst_ref=got_line,
        send_sem=ln_send,
        recv_sem=ln_recv,
        device_id={"seq": (seq + line) % n_seq},
        device_id_type=MESH,
    )
    pl.when(at_line < n_seq // line - 1)(line_copy.start)

    @pl.when(at_line > 0)
    def _():
        line_copy.wait_recv()

    @pl.when(at_line == 0)
    def _():
        got_line[...] = jnp.zeros_like(got_line)

    factor = jnp.ones((1, half), F32)
    earlier = got_line[...]
    for d in range(line):
        back_ref[d] = (inside[d] + factor * earlier).astype(BF16)
        factor = factor * decays_ref[8 * d : 8 * d + 1, :]

    def back_copy(k, owner):
        return pltpu.make_async_remote_copy(
            src_ref=back_ref.at[(place + k) % line],
            dst_ref=inc_ref.at[own_part(owner)],
            send_sem=bk_send.at[k],
            recv_sem=bk_recv.at[owner],
            device_id=line_peer(k),
            device_id_type=MESH,
        )

    @pl.loop(1, line)
    def _(i):
        back_copy(farthest_first(i), place).start()

    inc_ref[own_part(place)] = back_ref[place]

    for k in range(1, n_head):
        bc_copy(k, 1, (me + n_head - k) % n_head).wait_recv()
    for one in loads[6:9]:
        one.wait()
    skip = jnp.sum(jnp.where(own_lane, skip_ref[...], 0.0), axis=1, keepdims=True)
    skip_row = expand(jnp.broadcast_to(skip, (heads, 8)), spread, 3)[:1, :]

    @pl.loop(0, spans)
    def _(s):
        at = pl.ds(pl.multiple_of(s * SPAN, SPAN), SPAN)
        col, row, previous, _ = ids_of(s)
        c_here = ct_ref[:, at].T
        cn_ref[at, :] = c_here
        scores = jnp.dot(c_here, bt_ref[:, at], preferred_element_type=F32)
        seen = (col == row) & (iota((SPAN, SPAN), 0) >= iota((SPAN, SPAN), 1))
        scores = jnp.where(seen, scores, 0.0).astype(BF16)
        local = jnp.dot(scores, xf_ref[at, :], preferred_element_type=F32)
        inter = jnp.dot(c_here, before_ref[s].astype(BF16), preferred_element_type=F32)
        base = pl.multiple_of(s * 16, 16)
        out_of_middle = expand(e_ref[:, at], spread)
        from_start = rows_ref[pl.ds(base, 1), :] * jnp.where(col == previous, 1.0, 0.0)
        gate = z_ref[at, :].astype(F32)
        gate = gate / (1.0 + jnp.exp(-gate))
        y = out_of_middle * (local + from_start * inter) + skip_row * x_ref[at, :].astype(F32)
        ur_ref[at, :] = y * gate
        as_ref[at, :] = out_of_middle * from_start * gate

    loads[9].wait()

    @pl.loop(1, line)
    def _(k):
        back_copy(k, from_peer(k)).wait_recv()

    def finish(block):
        at = pl.ds(pl.multiple_of(block * SPAN, SPAN), SPAN)
        before = jnp.ones((1, width), F32)
        for s in range(spans - 1):
            decay = rows_ref[16 * s + 8 : 16 * s + 9, :]
            before = jnp.where(s + iota((1, width), 0) < block, before * decay, before)
        carried = (inc_ref[...].astype(F32) * before).astype(BF16)
        inter = jnp.dot(cn_ref[at, :], carried, preferred_element_type=F32)
        gated = ur_ref[at, :] + as_ref[at, :] * inter
        norm_ref[at, :] = (gated * gain_ref[...]).astype(BF16)
        squares = gated * gated
        folded = squares[:, :128]
        for j in range(1, width // 128):
            folded = folded + squares[:, 128 * j : 128 * (j + 1)]
        folded_ref[at, :] = folded

    def square_rows(block):
        folded = folded_ref[pl.ds(pl.multiple_of(block * SPAN, SPAN), SPAN), :]
        sq_ref[block] = jnp.broadcast_to(jnp.sum(folded.T, axis=0, keepdims=True), (8, SPAN))

    def square_copy(k, owner):
        return pltpu.make_async_remote_copy(
            src_ref=sq_ref.at[(me + k) % n_head],
            dst_ref=got_sq.at[owner],
            send_sem=sq_send.at[k],
            recv_sem=sq_recv.at[owner],
            device_id={"head": (me + k) % n_head},
            device_id_type=MESH,
        )

    out_width = out_ref.shape[1]
    parts, cut = got_r.shape[1], got_r.shape[3]

    def product(block, column):
        return jnp.dot(
            norm_ref[pl.ds(pl.multiple_of(block * SPAN, SPAN), SPAN), :],
            w_ref[:, pl.ds(pl.multiple_of(column, cut), cut)],
            preferred_element_type=F32,
        )

    def right_copy(step, j):
        return pltpu.make_async_remote_copy(
            src_ref=send_r.at[step, j],
            dst_ref=got_r.at[step, j],
            send_sem=r_send.at[step, j],
            recv_sem=r_recv.at[step, j],
            device_id={"head": (me + 1) % n_head},
            device_id_type=MESH,
        )

    def left_copy(step, j):
        return pltpu.make_async_remote_copy(
            src_ref=send_l.at[step, j],
            dst_ref=got_l.at[step, j],
            send_sem=l_send.at[step, j],
            recv_sem=l_recv.at[step, j],
            device_id={"head": (me + n_head - 1) % n_head},
            device_id_type=MESH,
        )

    ahead, behind = (me + n_head - 1) % n_head, (me + 1) % n_head
    def first_right(j):
        send_r[0, j] = product(ahead, j * cut).astype(BF16)
        right_copy(0, j).start()

    def first_left(j):
        send_l[0, j] = product(behind, out_width // 2 + j * cut).astype(BF16)
        left_copy(0, j).start()

    finish(ahead)
    first_right(0)
    finish(behind)
    first_left(0)

    @pl.loop(1, parts)
    def _(j):
        first_right(j)
        first_left(j)

    for k in range(2, n_head):
        finish((me + k) % n_head) if k < n_head - 1 else finish(me)
    for k in range(n_head):
        square_rows((me + k) % n_head)
    for k in range(1, n_head):
        square_copy(k, me).start()

    for step in range(1, n_head - 1):
        block_r, block_l = (me + 2 * n_head - 1 - step) % n_head, (me + 1 + step) % n_head

        @pl.loop(0, parts)
        def _(j):
            own = product(block_r, j * cut)
            right_copy(step - 1, j).wait_recv()
            send_r[step, j] = (own + got_r[step - 1, j].astype(F32)).astype(BF16)
            right_copy(step, j).start()
            own = product(block_l, out_width // 2 + j * cut)
            left_copy(step - 1, j).wait_recv()
            send_l[step, j] = (own + got_l[step - 1, j].astype(F32)).astype(BF16)
            left_copy(step, j).start()

    total = sq_ref[me]
    for k in range(1, n_head):
        owner = (me + n_head - k) % n_head
        square_copy(k, owner).wait_recv()
        total = total + got_sq[owner]
    inverse_rms = lax.rsqrt(total / (width * n_head) + NORM_EPS).T[:, :1]

    @pl.loop(0, parts)
    def _(j):
        last = n_head - 2
        own = product(me, j * cut)
        right_copy(last, j).wait_recv()
        own = (own + got_r[last, j].astype(F32)) * inverse_rms
        out_ref[:, pl.ds(pl.multiple_of(j * cut, cut), cut)] = own.astype(BF16)
        column = out_width // 2 + j * cut
        own = product(me, column)
        left_copy(last, j).wait_recv()
        own = (own + got_l[last, j].astype(F32)) * inverse_rms
        out_ref[:, pl.ds(pl.multiple_of(column, cut), cut)] = own.astype(BF16)

    for k in range(1, n_head):
        for what in range(2):
            bc_copy(k, what, me).wait_send()
        square_copy(k, me).wait_send()

    @pl.loop(1, line)
    def _(k):
        decay_copy(k, place).wait_send()
        state_copy(k, place).wait_send()
        back_copy(k, place).wait_send()

    pl.when(at_line < n_seq // line - 1)(line_copy.wait_send)
    for step in range(n_head - 1):

        @pl.loop(0, parts)
        def _(j):
            right_copy(step, j).wait_send()
            left_copy(step, j).wait_send()


def on_device(sizes, x_in, z_gate, b_in, c_in, dt_raw, decay_rate, skip_gain, norm_gain, w_out, doc_lengths):
    n_head, n_seq, line = sizes
    rows, width = x_in.shape
    heads = dt_raw.shape[1]
    out_width = w_out.shape[1]
    state_size = b_in.shape[1] * n_head
    spans = rows // SPAN
    part, half = state_size * 2 // line, width // 2
    parts = 5
    cut = out_width // 2 // parts
    ring = (n_head - 1, parts, rows // n_head, cut)
    vmem, anywhere = pl.BlockSpec(memory_space=pltpu.VMEM), pl.BlockSpec(memory_space=pl.ANY)
    dma = pltpu.SemaphoreType.DMA
    result = pl.pallas_call(
        functools.partial(layer_kernel, sizes),
        out_shape=pltpu.VMEM((rows // n_head, out_width), BF16),
        in_specs=[anywhere] * 10,
        out_specs=vmem,
        scratch_shapes=[
            pltpu.VMEM((state_size // n_head, rows), BF16),
            pltpu.VMEM((state_size // n_head, rows), BF16),
            pltpu.VMEM((heads, rows), F32),
            pltpu.VMEM((1, heads), F32),
            pltpu.VMEM((1, heads), F32),
            pltpu.VMEM((1, width), F32),
            pltpu.VMEM((1, doc_lengths.shape[0]), jnp.int32),
            pltpu.VMEM((rows, width), BF16),
            pltpu.VMEM((rows, width), BF16),
            pltpu.VMEM(w_out.shape, BF16),
            pltpu.VMEM((state_size, rows), BF16),
            pltpu.VMEM((state_size, rows), BF16),
            pltpu.VMEM((rows, width), BF16),
            pltpu.VMEM((heads, rows), F32),
            pltpu.VMEM((spans * 16, width), F32),
            pltpu.VMEM((spans, state_size, width), F32),
            pltpu.VMEM((rows, width), F32),
            pltpu.VMEM((rows, width), F32),
            pltpu.VMEM((state_size, width), BF16),
            pltpu.VMEM((8, 128), F32),
            pltpu.VMEM((line, part, half), BF16),
            pltpu.VMEM((line, 8, 128), F32),
            pltpu.VMEM((part, half), F32),
            pltpu.VMEM((part, half), F32),
            pltpu.VMEM((line, part, half), BF16),
            pltpu.VMEM((state_size, width), BF16),
            pltpu.VMEM((rows, width), BF16),
            pltpu.VMEM((n_head, 8, SPAN), F32),
            pltpu.VMEM((n_head, 8, SPAN), F32),
            pltpu.VMEM(ring, BF16),
            pltpu.VMEM(ring, BF16),
            pltpu.VMEM(ring, BF16),
            pltpu.VMEM(ring, BF16),
            pltpu.VMEM((line * 8, half), F32),
            pltpu.VMEM((rows, state_size), BF16),
            pltpu.VMEM((rows, 128), F32),
            pltpu.VMEM((state_size, rows), BF16),
            dma((10,)),
            dma((2, n_head)),
            dma((2, n_head)),
            dma((line,)),
            dma((line,)),
            dma((line,)),
            dma((line,)),
            dma,
            dma,
            dma((line,)),
            dma((line,)),
            dma((n_head,)),
            dma((n_head,)),
            dma((n_head - 1, parts)),
            dma((n_head - 1, parts)),
            dma((n_head - 1, parts)),
            dma((n_head - 1, parts)),
        ],
        compiler_params=pltpu.CompilerParams(
            collective_id=0, has_side_effects=True, vmem_limit_bytes=60 * 1024 * 1024
        ),
        name="ssd_layer",
    )(
        b_in.T,
        c_in.T,
        dt_raw.T,
        decay_rate[None, :],
        skip_gain[None, :],
        norm_gain[None, :],
        doc_lengths[None, :],
        x_in,
        z_gate,
        w_out,
    )
    return result


def solution(mesh):
    sizes = (mesh.shape["head"], mesh.shape["seq"], 16)
    rows = P("seq", "head")
    return jax.shard_map(
        functools.partial(on_device, sizes),
        mesh=mesh,
        in_specs=(rows, rows, rows, rows, rows, P("head"), P("head"), P("head"), P("head", None), P()),
        out_specs=P(("seq", "head"), None),
        check_vma=False,
    )
```
